128 devices in a mesh: mesh: 2 (over core), dom: 64 (over z, x, y).
Axes of the slice: x: 4, y: 4, z: 4, core: 2. Of those that a mesh axis runs over, the one named last changes fastest.
Arguments:
- donor_fields: float32 [5, 512, 16384], P(None, None, ('mesh', 'dom')), may hold values from -6 to 6
- interp_weights: float32 [3, 8, 262144], P(None, None, ('mesh', 'dom')), may hold values from -1 to 1, as said below
- donor_owner: int32 [262144, 1], P(('mesh', 'dom')), may hold values from 0 to 63, as said below
- donor_element: int32 [262144], P(('mesh', 'dom')), may hold values from 0 to 127
- geometry: float32 [4, 16384], P(None, ('mesh', 'dom')), may hold values from 0.25 to 4
- wall_flag: int32 [2, 1024], P(None, ('mesh', 'dom')), may hold values 0 or 1
- forcing: float32 [512, 16384], P(None, ('mesh', 'dom')), may hold values from -6 to 6
Outputs:
- velocity: float32 [512, 16384], P(None, ('mesh', 'dom'))
- residual: float32 [512, 16384], P(None, ('mesh', 'dom'))
- interface_values: float32 [5, 262144], P(None, ('mesh', 'dom'))
The draws below stay inside these ranges and needn't reach their ends.
Inputs may be any that keep to these rules, and one draw needn't show every extreme that they name: `interp_weights`: for each receptor and direction, the 8 entries are the Lagrange polynomials of the order-7 Gauss-Lobatto-Legendre points evaluated at one point of [-1, 1]. `donor_owner`: the receptors of block q of a mesh (the rows of one device) name donor dom indices from q - 2 to q + 2 only; among them one index is named exactly 1024 times and no index more often.
All inputs are finite; a program needn't handle non-finite values. No bound on the sum of `wall_flag` on one device may be relied on, other than what follows from the above.
Results may differ from the reference program's by a relative error of at most 0.00026.
Values sent between devices are 32-bit elements; how exact they have to be, the bound alone decides.
A program may use at most 192 MiB of HBM per device.

```python
import math
import jax
import jax.numpy as jnp
import numpy as np
from jax import lax

FIELDS = 5
EX = 8
EY = 16
EZ_DEV = 1
ITERS = 3
PTS = 512
E_DEV = 128
E_TOTAL = 16384
R_DEV = 2048
R_TOTAL = 262144
CAP = 1024
W_TOTAL = 1024
N_MESH = 2
N_DOM = 64


def legendre_pair_drawn(values, degree):
    previous = values * 0.0 + 1.0
    current = values * 1.0
    for poly_order in range(2, degree + 1):
        previous, current = (current, ((2 * poly_order - 1) * values * current - (poly_order - 1) * previous) / poly_order)
    return (current, previous)


def gll_abscissae():
    degree = 7
    points_count = degree + 1
    abscissae = np.cos(np.pi * np.arange(points_count) / degree)
    for newton_turn in range(80):
        top_poly, lower_poly = legendre_pair_drawn(abscissae, degree)
        abscissae = abscissae - (abscissae * top_poly - lower_poly) / (points_count * top_poly)
    return np.sort(abscissae)


def draw_interp_weights(key, part):
    abscissae = gll_abscissae()
    location = jax.random.uniform(key, (3, R_TOTAL), jnp.float32, -1.0, 1.0)
    basis_rows = []
    for node_index in range(8):
        product = jnp.ones_like(location)
        for partner in range(8):
            if partner != node_index:
                product = product * (location - abscissae[partner]) / (abscissae[node_index] - abscissae[partner])
        basis_rows.append(product)
    return jnp.stack(basis_rows, 1).astype(jnp.float32)


def draw_donor_owner(key, part):
    block_count = N_MESH * N_DOM
    slab_index = jnp.arange(block_count, dtype=jnp.int32) % N_DOM
    lowest = jnp.maximum(slab_index - 2, 0)
    highest = jnp.minimum(slab_index + 2, N_DOM - 1)
    window = highest - lowest + 1
    hot_owner = lowest + jax.random.randint(jax.random.fold_in(key, 11), (block_count,), 0, window)
    picks = jax.random.randint(jax.random.fold_in(key, 13), (block_count, R_DEV), 0, (window - 1)[:, None])
    other_owner = lowest[:, None] + picks
    other_owner = other_owner + (other_owner >= hot_owner[:, None]).astype(jnp.int32)
    block_keys = jax.random.split(jax.random.fold_in(key, 17), block_count)
    ranks = jax.vmap(lambda one_key: jax.random.permutation(one_key, R_DEV))(block_keys)
    owner = jnp.where(ranks < CAP, hot_owner[:, None], other_owner)
    return owner.reshape(R_TOTAL, 1).astype(jnp.int32)


def place_ends(values, own_key, smallest, largest):
    index_at = [jax.random.randint(jax.random.fold_in(own_key, axis), (), 0, length) for axis, length in enumerate(values.shape)]
    main_axis = values.shape.index(max(values.shape))
    next_to = index_at[:main_axis] + [(index_at[main_axis] + 1) % values.shape[main_axis]] + index_at[main_axis + 1:]
    return values.at[tuple(index_at)].set(smallest).at[tuple(next_to)].set(largest)


def shard_levels(own_key, shape, pieces, least, top_value):
    loudness = 1.0
    for axis_at, blocks in pieces:
        draws = jax.random.uniform(jax.random.fold_in(jax.random.fold_in(own_key, 6), axis_at), (blocks,), jnp.float32, least / len(pieces), top_value / len(pieces))
        loudness = loudness * jnp.repeat(jnp.exp(draws), shape[axis_at] // blocks).reshape((-1,) + (1,) * (len(shape) - 1 - axis_at))
    return loudness


def noise(key, dims, deviation, bound, shards=(), kind=jnp.bfloat16):
    values = jax.random.normal(key, dims, jnp.float32) * deviation
    if len(shards) > 0:
        values = shard_levels(key, dims, shards, -0.22, 0.18) * values
    return jnp.clip(values, min=-bound, max=bound).astype(kind)


def setup_inputs(seed: int = 0) -> dict:
    seeds = jax.random.split(jax.random.key(seed), 8)
    donor_fields = noise(seeds[0], (FIELDS, PTS, E_TOTAL), 1.0, 6.0, ((2, 128),), jnp.float32)
    interp_weights = draw_interp_weights(jax.random.fold_in(seeds[7], 71), 0)
    donor_owner = draw_donor_owner(jax.random.fold_in(seeds[7], 71), 0)
    donor_element = place_ends(jax.random.randint(seeds[3], (R_TOTAL,), 0, E_DEV), jax.random.fold_in(seeds[3], 1), 0, E_DEV - 1).astype(jnp.int32)
    geometry = jnp.clip(jnp.exp(math.log(4.0) - 2.7725887 * jax.random.uniform(seeds[4], (4, E_TOTAL), jnp.float32) ** shard_levels(seeds[4], (4, E_TOTAL), ((1, 128),), -0.2, 0.2)), 0.25, 4.0)
    wall_flag = place_ends((jax.random.randint(seeds[5], (2, W_TOTAL), 0, 4) < 3).astype(jnp.int32), jax.random.fold_in(seeds[5], 1), 0, 1)
    forcing = noise(seeds[6], (PTS, E_TOTAL), 1.0, 6.0, ((1, 128),), jnp.float32)
    return {"donor_fields": donor_fields, "interp_weights": interp_weights, "donor_owner": donor_owner, "donor_element": donor_element, "geometry": geometry, "wall_flag": wall_flag, "forcing": forcing}


HIGHEST = lax.Precision.HIGHEST


def legendre_pair(values, degree):
    previous = values * 0.0 + 1.0
    current = values * 1.0
    for poly_order in range(2, degree + 1):
        previous, current = current, ((2 * poly_order - 1) * values * current - (poly_order - 1) * previous) / poly_order
    return current, previous


def gll_tables():
    degree = 7
    points_count = degree + 1
    abscissae = np.cos(np.pi * np.arange(points_count) / degree)
    for newton_turn in range(80):
        top_poly, lower_poly = legendre_pair(abscissae, degree)
        abscissae = abscissae - (abscissae * top_poly - lower_poly) / (points_count * top_poly)
    abscissae = np.sort(abscissae)
    top_poly, lower_poly = legendre_pair(abscissae, degree)
    quad_weights = 2.0 / (degree * points_count * top_poly * top_poly)
    identity_mat = np.eye(points_count)
    spacing = abscissae[:, None] - abscissae[None, :] + identity_mat
    derivative = (top_poly[:, None] / (top_poly[None, :] * spacing)) * (1.0 - identity_mat)
    derivative[0, 0] = -degree * points_count / 4.0
    derivative[degree, degree] = degree * points_count / 4.0
    return jnp.asarray(derivative, jnp.float32), jnp.asarray(quad_weights, jnp.float32)


def cube_weights(quad_weights):
    return quad_weights[:, None, None, None] * quad_weights[None, :, None, None] * quad_weights[None, None, :, None]


def local_operator(field_data, geometry, derivative, quad_weights):
    weights_cube = cube_weights(quad_weights)
    grad_x = jnp.einsum('ai,kjie->kjae', derivative, field_data, precision=HIGHEST)
    grad_y = jnp.einsum('aj,kjie->kaie', derivative, field_data, precision=HIGHEST)
    grad_z = jnp.einsum('ak,kjie->ajie', derivative, field_data, precision=HIGHEST)
    result = jnp.einsum('ai,kjae->kjie', derivative, grad_x * (weights_cube * geometry[0]), precision=HIGHEST)
    result = result + jnp.einsum('aj,kaie->kjie', derivative, grad_y * (weights_cube * geometry[1]), precision=HIGHEST)
    result = result + jnp.einsum('ak,ajie->kjie', derivative, grad_z * (weights_cube * geometry[2]), precision=HIGHEST)
    return result + (weights_cube * geometry[3]) * field_data


def local_diagonal(geometry, derivative, quad_weights):
    stiff_diag = jnp.sum(derivative * derivative * quad_weights[:, None], axis=0)
    along_x = (quad_weights[:, None, None] * quad_weights[None, :, None] * stiff_diag[None, None, :])[..., None]
    along_y = (quad_weights[:, None, None] * stiff_diag[None, :, None] * quad_weights[None, None, :])[..., None]
    along_z = (stiff_diag[:, None, None] * quad_weights[None, :, None] * quad_weights[None, None, :])[..., None]
    return along_x * geometry[0] + along_y * geometry[1] + along_z * geometry[2] + cube_weights(quad_weights) * geometry[3]


def direct_sum(field_data):
    paired = field_data[:, :, :, -1, :, :, :-1] + field_data[:, :, :, 0, :, :, 1:]
    field_data = field_data.at[:, :, :, -1, :, :, :-1].set(paired).at[:, :, :, 0, :, :, 1:].set(paired)
    paired = field_data[:, :, -1, :, :, :-1, :] + field_data[:, :, 0, :, :, 1:, :]
    field_data = field_data.at[:, :, -1, :, :, :-1, :].set(paired).at[:, :, 0, :, :, 1:, :].set(paired)
    paired = field_data[:, -1, :, :, :-1, :, :] + field_data[:, 0, :, :, 1:, :, :]
    field_data = field_data.at[:, -1, :, :, :-1, :, :].set(paired).at[:, 0, :, :, 1:, :, :].set(paired)
    return field_data


def reference(donor_fields, interp_weights, donor_owner, donor_element, geometry, wall_flag, forcing):
    derivative, quad_weights = gll_tables()
    elem_dev = EX * EY * EZ_DEV
    elem_mesh = elem_dev * N_DOM
    rec_mesh = R_DEV * N_DOM
    layers = EZ_DEV * N_DOM
    receptor_mesh = jnp.arange(R_TOTAL, dtype=jnp.int32) // rec_mesh
    target = ((1 - receptor_mesh) * elem_mesh + donor_owner[:, 0] * elem_dev + donor_element).astype(jnp.int32)
    blocks = N_MESH * N_DOM
    target_blocks = target.reshape(blocks, R_DEV)
    weight_blocks = jnp.transpose(interp_weights.reshape(3, 8, blocks, R_DEV), (2, 0, 1, 3))

    def evaluate(block_pair):
        target_row, weight_row = block_pair
        gathered = jnp.take(donor_fields, target_row, axis=2).reshape(FIELDS, 8, 8, 8, R_DEV)
        reduced = jnp.einsum('fkjib,ib->fkjb', gathered, weight_row[0], precision=HIGHEST)
        reduced = jnp.einsum('fkjb,jb->fkb', reduced, weight_row[1], precision=HIGHEST)
        return jnp.einsum('fkb,kb->fb', reduced, weight_row[2], precision=HIGHEST)

    evaluated = lax.map(evaluate, (target_blocks, weight_blocks))
    interface_values = jnp.transpose(evaluated, (1, 0, 2)).reshape(FIELDS, R_TOTAL)

    brick_shape = (8, 8, 8, layers, EY, EX)
    flat_shape = (8, 8, 8, elem_mesh)
    weights_cube = cube_weights(quad_weights)
    velocities = []
    residuals = []
    for mesh_index in range(N_MESH):
        first_column = mesh_index * elem_mesh
        mesh_geometry = geometry[:, first_column:first_column + elem_mesh]
        source = forcing[:, first_column:first_column + elem_mesh].reshape(flat_shape)
        received = interface_values[0, mesh_index * rec_mesh:(mesh_index + 1) * rec_mesh]
        received = received.reshape(N_DOM, 2, EZ_DEV, EY, 8, 8)
        side_values = jnp.transpose(received, (1, 4, 5, 0, 2, 3)).reshape(2, 8, 8, layers, EY)
        wall_bits = wall_flag[:, mesh_index * EX * layers:(mesh_index + 1) * EX * layers].reshape(2, layers, EX)
        wall_bits = wall_bits.astype(jnp.float32)
        zero_brick = jnp.zeros(brick_shape, jnp.float32)
        rec_value = zero_brick.at[:, :, 0, :, :, 0].set(side_values[0]).at[:, :, -1, :, :, -1].set(side_values[1])
        rec_mark = zero_brick.at[:, :, 0, :, :, 0].set(1.0).at[:, :, -1, :, :, -1].set(1.0)
        wall_low = jnp.broadcast_to(wall_bits[0], (8, 8, layers, EX))
        wall_high = jnp.broadcast_to(wall_bits[1], (8, 8, layers, EX))
        wall_mark = zero_brick.at[:, 0, :, :, 0, :].set(wall_low).at[:, -1, :, :, -1, :].set(wall_high)
        diag_brick = local_diagonal(mesh_geometry, derivative, quad_weights).reshape(brick_shape)
        unit_brick = jnp.ones(brick_shape, jnp.float32)
        summed = direct_sum(jnp.stack([rec_value, rec_mark, wall_mark, unit_brick, diag_brick], 0))
        summed = summed.reshape((5,) + flat_shape)
        free_mask = 1.0 - jnp.minimum(summed[1] + summed[2], 1.0)
        boundary = summed[0] / jnp.maximum(summed[1], 1.0)
        multiplicity = summed[3]
        inverse = free_mask / summed[4]

        def apply_operator(vector):
            local_term = local_operator(vector, mesh_geometry, derivative, quad_weights)
            return free_mask * direct_sum(local_term.reshape((1,) + brick_shape))[0].reshape(flat_shape)

        def inner(left, right):
            return jnp.sum(left * right / multiplicity)

        loaded = (weights_cube * mesh_geometry[3]) * source - local_operator(boundary, mesh_geometry, derivative, quad_weights)
        rhs = free_mask * direct_sum(loaded.reshape((1,) + brick_shape))[0].reshape(flat_shape)
        solution = jnp.zeros(flat_shape, jnp.float32)
        residual_now = rhs
        precond = inverse * residual_now
        direction = precond
        precond_norm = inner(residual_now, precond)
        for iteration in range(ITERS):
            operator_image = apply_operator(direction)
            step_length = precond_norm / inner(direction, operator_image)
            solution = solution + step_length * direction
            residual_now = residual_now - step_length * operator_image
            if iteration + 1 < ITERS:
                precond = inverse * residual_now
                norm_next = inner(residual_now, precond)
                direction = precond + (norm_next / precond_norm) * direction
                precond_norm = norm_next
        velocities.append((boundary + solution).reshape(PTS, elem_mesh))
        residuals.append(residual_now.reshape(PTS, elem_mesh))
    return jnp.concatenate(velocities, 1), jnp.concatenate(residuals, 1), interface_values
```

```python
import functools

import jax
import jax.numpy as jnp
import numpy as np
from jax import lax
from jax.experimental import pallas as pl
from jax.experimental.pallas import tpu as pltpu
from jax.sharding import PartitionSpec as P

MESH = pl.DeviceIdType.MESH
F32 = jnp.float32
NQ = 64
NB = 80


def legendre_pair(values, degree):
    previous = values * 0.0 + 1.0
    current = values * 1.0
    for order in range(2, degree + 1):
        previous, current = (
            current,
            ((2 * order - 1) * values * current - (order - 1) * previous) / order,
        )
    return current, previous


def gll():
    degree, count = 7, 8
    x = np.cos(np.pi * np.arange(count) / degree)
    for _ in range(80):
        top, lower = legendre_pair(x, degree)
        x = x - (x * top - lower) / (count * top)
    x = np.sort(x)
    top, _ = legendre_pair(x, degree)
    w = 2.0 / (degree * count * top * top)
    eye = np.eye(count)
    d = top[:, None] / (top[None, :] * (x[:, None] - x[None, :] + eye)) * (1.0 - eye)
    d[0, 0] = -degree * count / 4.0
    d[7, 7] = degree * count / 4.0
    return x, w, d


X, WQ, D = gll()
KP = (D.T * WQ[None, :]) @ D / WQ[:, None]
KP = 0.5 * (KP + KP[::-1, ::-1])
KE = 0.5 * (KP[:4, :4] + KP[:4, 7:3:-1])
KO = 0.5 * (KP[:4, :4] - KP[:4, 7:3:-1])
LC = np.array([1.0 / np.prod([X[n] - X[m] for m in range(8) if m != n]) for n in range(8)])


def const_table():
    lane = np.arange(128)
    xl = lane % 8
    rows = []
    rows.append(np.repeat(X[:, None], 128, 1))
    rows.append(np.repeat(WQ[:, None], 128, 1))
    for s in range(8):
        rows.append(np.repeat(np.array([KP[i, (i + s) % 8] for i in range(8)])[:, None], 128, 1))
    kx = np.zeros((8, 128))
    for i in range(8):
        kx[i] = np.where(xl == 0, KP[i, 0], np.where(xl == 7, KP[i, 7], 0.0))
    kx[0] = np.where(xl == 1, KP[7, 0], kx[0])
    kx[7] = np.where(xl == 6, KP[0, 7], kx[7])
    rows.append(kx)
    rows.append((np.arange(8)[:, None] == xl[None, :]).astype(float))
    return np.concatenate(rows, 0).astype(np.float32)


def kernel(
    donor_hbm, wts, owner, elem, geo, wall, forc_hbm, ct,
    vel, res, iv,
    donor, forc, req_src, req, aux_src, aux, W, IDX, ans_src, ans,
    FB, OUT, R0, INV, V, WA, DG, ND, QB, face_src, face, halo, ar,
    in_sem, req_s, req_r, aux_s, aux_r, ans_s, ans_r, face_s, face_r, halo_s, halo_r, ar_s, ar_r,
):
    m = lax.axis_index("mesh")
    q = lax.axis_index("dom")
    om = 1 - m
    barrier = pltpu.get_barrier_semaphore()

    def there(d):
        return jnp.logical_and(q + d >= 0, q + d < NQ)

    for d, s in ((-1, 0), (1, 1)):
        @pl.when(jnp.logical_not(there(d)))
        def _(s=s):
            aux[s] = jnp.zeros((8, 128), F32)
            face[s] = jnp.zeros((8, 128), F32)
            for r in range(4):
                halo[r, s] = jnp.zeros((64, 128), F32)
    for d in (-2, -1, 1, 2):
        @pl.when(jnp.logical_not(there(d)))
        def _(d=d):
            req[2 - d] = jnp.zeros((64, 128), F32)
            ans[2 + d] = jnp.zeros((5, 16, 128), F32)

    in_donor = pltpu.make_async_copy(donor_hbm, donor, in_sem.at[0])
    in_forc = pltpu.make_async_copy(forc_hbm, forc, in_sem.at[1])
    in_forc.start()
    in_donor.start()

    def greet(d, c):
        peer = lax.rem(q + d, NQ)
        pl.semaphore_signal(barrier, inc=1, device_id=(m, peer), device_id_type=MESH)
        return c

    lax.fori_loop(1, NQ, greet, 0)
    for d in range(-2, 3):
        @pl.when(there(d))
        def _(d=d):
            pl.semaphore_signal(barrier, inc=1, device_id=(om, q + d), device_id_type=MESH)

    i0 = lax.broadcasted_iota(jnp.int32, (8, 128), 0)
    lane = lax.broadcasted_iota(jnp.int32, (8, 128), 1)
    xl = lane & 7
    yl = lane >> 3
    xcol = ct[0:8, :]
    wcol = ct[8:16, :]

    for d in range(3):
        for b in range(16):
            t = wts[d, :, b * 128 : (b + 1) * 128] * xcol
            req_src[d * 16 + b : d * 16 + b + 1, :] = jnp.sum(t, axis=0, keepdims=True)
    req_src[48:64, :] = (owner[...] * 128 + elem[...]).astype(F32)
    aux_src[0:4, :] = geo[...]
    aux_src[4:6, :] = jnp.dot(
        wall[...].astype(F32), ct[88:96, :], preferred_element_type=F32
    )
    aux_src[6:8, :] = jnp.zeros((2, 128), F32)

    width = sum(there(d).astype(jnp.int32) for d in range(-2, 3))
    pl.semaphore_wait(barrier, NQ - 1 + width)

    def req_copy(d):
        return pltpu.make_async_remote_copy(
            req_src, req.at[d + 2], req_s.at[d + 2], req_r.at[d + 2],
            device_id=(om, q + d), device_id_type=MESH)

    def aux_copy(d):
        s = (d + 1) // 2
        return pltpu.make_async_remote_copy(
            aux_src, aux.at[1 - s], aux_s.at[s], aux_r.at[1 - s],
            device_id=(m, q + d), device_id_type=MESH)

    def face_copy(d):
        s = (d + 1) // 2
        return pltpu.make_async_remote_copy(
            face_src.at[s], face.at[1 - s], face_s.at[s], face_r.at[1 - s],
            device_id=(m, q + d), device_id_type=MESH)

    def halo_copy(src, r, d):
        s = (d + 1) // 2
        return pltpu.make_async_remote_copy(
            src.at[pl.ds(s * 448, 64)], halo.at[r, 1 - s], halo_s.at[r, s], halo_r.at[r, 1 - s],
            device_id=(m, q + d), device_id_type=MESH)

    def ans_copy(f, s):
        d = 2 - s
        return pltpu.make_async_remote_copy(
            ans_src.at[f, pl.ds(s * 16, 16)], ans.at[s, f], ans_s.at[f, s], ans_r.at[f, s],
            device_id=(om, q + d), device_id_type=MESH)

    def when_there(d, act):
        @pl.when(there(d))
        def _():
            act()

    for d in (2, -2, 1, -1, 0):
        when_there(d, lambda d=d: req_copy(d).start())
    for d in (-1, 1):
        when_there(d, lambda d=d: aux_copy(d).start())

    m7x = jnp.logical_and(i0 == 7, xl < 7)
    m0x = jnp.logical_and(i0 == 0, xl > 0)
    m7y = jnp.logical_and(i0 == 7, yl < 15)
    m0y = jnp.logical_and(i0 == 0, yl > 0)
    xhi, xlo = xl < 7, xl > 0
    yhi, ylo = yl < 15, yl > 0

    def sum_xy(ref, base, planes):
        for k in range(planes):
            lo = ref[pl.ds(base + k * 64, 8, stride=8), :]
            hi = ref[pl.ds(base + k * 64 + 7, 8, stride=8), :]
            ref[pl.ds(base + k * 64, 8, stride=8), :] = lo + jnp.where(
                xlo, pltpu.roll(hi, 1, axis=1), 0.0)
            ref[pl.ds(base + k * 64 + 7, 8, stride=8), :] = hi + jnp.where(
                xhi, pltpu.roll(lo, 127, axis=1), 0.0)
        for k in range(planes):
            at = base + k * 64
            lo = ref[at : at + 8, :]
            hi = ref[at + 56 : at + 64, :]
            ref[at : at + 8, :] = lo + jnp.where(ylo, pltpu.roll(hi, 8, axis=1), 0.0)
            ref[at + 56 : at + 64, :] = hi + jnp.where(yhi, pltpu.roll(lo, 120, axis=1), 0.0)

    def rows(ref, n):
        return jnp.broadcast_to(ref[n : n + 1, :], (8, 128))

    g0, g1, g2, g3 = (rows(geo, n) for n in range(4))

    def tile(k, j):
        at = (k * 8 + j) * 8
        return slice(at, at + 8)

    def wkj(k, j):
        return float(WQ[k] * WQ[j])

    in_forc.wait()
    g3w = g3 * wcol
    for k in range(8):
        for j in range(8):
            FB[tile(k, j), :] = forc[tile(k, j), :] * (g3w * wkj(k, j))
    sum_xy(FB, 0, 8)
    for d in (-1, 1):
        when_there(d, lambda d=d: halo_copy(FB, 0, d).start())

    for d, s in ((-1, 0), (1, 1)):
        when_there(d, lambda d=d, s=s: aux_copy(-d).wait_recv())

    plane = jnp.logical_or(
        jnp.logical_and(i0 == 0, xl == 0), jnp.logical_and(i0 == 7, xl == 7))
    pm = jnp.where(plane, 0.0, 1.0)

    def wall_count(row):
        return (row + jnp.where(m7x, pltpu.roll(row, 127, axis=1), 0.0)
                + jnp.where(m0x, pltpu.roll(row, 1, axis=1), 0.0))

    masks = {}
    for n, (j, edge) in enumerate(((0, yl == 0), (7, yl == 15))):
        own = wall_count(rows(aux_src, 4 + n))
        below = wall_count(jnp.broadcast_to(aux[0, 4 + n : 5 + n, :], (8, 128)))
        above = wall_count(jnp.broadcast_to(aux[1, 4 + n : 5 + n, :], (8, 128)))
        for name, count in (("lo", own + below), ("in", own), ("hi", own + above)):
            masks[j, name] = pm * (1.0 - jnp.where(edge, jnp.minimum(count, 1.0), 0.0))

    def free(k, j):
        if j not in (0, 7):
            return pm
        return masks[j, "lo" if k == 0 else "hi" if k == 7 else "in"]

    kdiag = ct[16:24, :]

    def diag_tile(h0, h1, h2, h3, k, j):
        return (h0 * kdiag + h1 * float(KP[j, j]) + h2 * float(KP[k, k]) + h3) * (
            wcol * wkj(k, j))

    for k in range(8):
        for j in range(8):
            DG[tile(k, j), :] = diag_tile(g0, g1, g2, g3, k, j)
    for s in range(2):
        h = [jnp.broadcast_to(aux[s, n : n + 1, :], (8, 128)) for n in range(4)]
        for j in range(8):
            ND[s * 64 + j * 8 : s * 64 + j * 8 + 8, :] = diag_tile(*h, 0, j)
    sum_xy(DG, 0, 8)
    sum_xy(ND, 0, 2)
    for k in range(8):
        for j in range(8):
            value = DG[tile(k, j), :]
            if k == 0:
                value = value + ND[tile(0, j), :]
            if k == 7:
                value = value + ND[tile(1, j), :]
            INV[tile(k, j), :] = free(k, j) / value

    in_donor.wait()

    def weights(s):
        for h in range(2):
            at = s * 16 + 8 * h
            code = req[s, 48 + 8 * h : 56 + 8 * h, :] - (q * 128).astype(F32)
            mine = jnp.logical_and(code >= 0.0, code < 128.0)
            IDX[at : at + 8, :] = jnp.where(mine, code, 0.0).astype(jnp.int32)
            keep = jnp.where(mine, 1.0, 0.0)
            for d in range(3):
                xi = req[s, d * 16 + 8 * h : d * 16 + 8 * h + 8, :]
                t = [xi - float(X[n]) for n in range(8)]
                pre, suf = [None], [None] * 8
                for n in range(1, 8):
                    pre.append(t[n - 1] if n == 1 else pre[-1] * t[n - 1])
                for n in range(6, -1, -1):
                    suf[n] = t[7] if n == 6 else suf[n + 1] * t[n + 1]
                for n in range(8):
                    a = suf[0] if n == 0 else pre[7] if n == 7 else pre[n] * suf[n]
                    a = a * float(LC[n])
                    if d == 0:
                        a = a * keep
                    W[(d * 8 + n) * NB + at : (d * 8 + n) * NB + at + 8, :] = a

    def evaluate(f, first, count, unroll):
        def block(b):
            idx = jnp.broadcast_to(IDX[pl.ds(b, 1), :], (8, 128))
            wi = W[pl.ds(b, 8, stride=NB), :]
            total = None
            for k in range(8):
                wk = jnp.broadcast_to(W[pl.ds((16 + k) * NB + b, 1), :], (8, 128))
                part = None
                for j in range(8):
                    wj = jnp.broadcast_to(W[pl.ds((8 + j) * NB + b, 1), :], (8, 128))
                    g = jnp.take_along_axis(
                        donor[f, tile(k, j), :], idx, axis=1, mode="promise_in_bounds")
                    part = g * wj if part is None else part + g * wj
                total = part * wk if total is None else total + part * wk
            ans_src[f, pl.ds(b, 1), :] = jnp.sum(total * wi, axis=0, keepdims=True)

        def step(n, c):
            for u in range(unroll):
                block(first + n * unroll + u)
            return c

        lax.fori_loop(0, count // unroll, step, 0)

    def send_field(f):
        for s in (0, 4, 1, 3, 2):
            when_there(2 - s, lambda s=s: ans_copy(f, s).start())

    for s in (2, 1, 3, 0, 4):
        when_there(2 - s, lambda s=s: req_copy(s - 2).wait_recv())
        weights(s)
        evaluate(0, s * 16, 16, 8)
        when_there(2 - s, lambda s=s: ans_copy(0, s).start())

    evaluate(1, 0, NB, 8)
    send_field(1)

    for s in range(5):
        when_there(s - 2, lambda s=s: ans_copy(0, s).wait_recv())
    got = ans[0, 0] + ans[1, 0] + ans[2, 0] + ans[3, 0] + ans[4, 0]
    turned = jnp.transpose(jnp.concatenate([got, jnp.zeros((112, 128), F32)], 0))
    column = jnp.where(xl == 7, 8, 0) + (yl >> 1)
    even = (yl & 1) == 0
    ends = jnp.logical_or(xl == 0, xl == 7)
    T = []
    for k in range(8):
        a = jnp.take_along_axis(turned[k * 8 : k * 8 + 8, :], column, axis=1,
                                mode="promise_in_bounds")
        b = jnp.take_along_axis(turned[64 + k * 8 : 72 + k * 8, :], column, axis=1,
                                mode="promise_in_bounds")
        t = jnp.where(ends, jnp.where(even, a, b), 0.0)
        T.append(t + jnp.where(m7y, pltpu.roll(pltpu.roll(t, 120, axis=1), 7, axis=0), 0.0)
                 + jnp.where(m0y, pltpu.roll(pltpu.roll(t, 8, axis=1), 1, axis=0), 0.0))
    face_src[0] = T[0]
    face_src[1] = T[7]
    for d in (-1, 1):
        when_there(d, lambda d=d: face_copy(d).start())

    evaluate(2, 0, NB, 8)
    send_field(2)

    for d in (-1, 1):
        when_there(d, lambda d=d: face_copy(-d).wait_recv())
    T[0] = T[0] + face[0]
    T[7] = T[7] + face[1]
    czd = jnp.where(q > 0, 0.5, 1.0).astype(F32)
    czu = jnp.where(q < NQ - 1, 0.5, 1.0).astype(F32)
    cyv = jnp.where(jnp.logical_or(m7y, m0y), 0.5, 1.0)

    def spread_y(row):
        return (row + jnp.where(m7y, pltpu.roll(row, 120, axis=1), 0.0)
                + jnp.where(m0y, pltpu.roll(row, 8, axis=1), 0.0))

    gy = spread_y(g0)
    gy_below = spread_y(jnp.broadcast_to(aux[0, 0:1, :], (8, 128)))
    gy_above = spread_y(jnp.broadcast_to(aux[1, 0:1, :], (8, 128)))
    for k in range(8):
        b = T[k] * cyv
        gs = gy
        if k == 0:
            b, gs = b * czd, gs + gy_below
        if k == 7:
            b, gs = b * czu, gs + gy_above
        QB[64 + k * 8 : 72 + k * 8, :] = b
        t = b * gs
        t = jnp.where(xl == 1, pltpu.roll(t, 1, axis=1),
                      jnp.where(xl == 6, pltpu.roll(t, 127, axis=1), t))
        QB[k * 8 : k * 8 + 8, :] = t

    cx = jnp.where(jnp.logical_or(m7x, m0x), 0.5, 1.0)
    cxy = {0: cx * jnp.where(ylo, 0.5, 1.0), 7: cx * jnp.where(yhi, 0.5, 1.0)}

    def assembled(src, r, k, j):
        value = src[tile(k, j), :]
        if k == 0:
            value = value + halo[r, 0, j * 8 : j * 8 + 8, :]
        if k == 7:
            value = value + halo[r, 1, j * 8 : j * 8 + 8, :]
        return value

    def wait_halo(src, r):
        for d in (-1, 1):
            when_there(d, lambda d=d: halo_copy(src, r, -d).wait_recv())

    def product_sum(make):
        total = None
        for k in range(8):
            part = None
            for j in range(8):
                t = make(k, j) * cxy.get(j, cx)
                part = t if part is None else part + t
            if k == 0:
                part = part * czd
            if k == 7:
                part = part * czu
            total = part if total is None else total + part
        return total

    kxw = ct[80:88, :] * wcol
    wait_halo(FB, 0)

    def first(k, j):
        value = assembled(FB, 0, k, j) - rows(QB, k * 8 + j) * (kxw * wkj(k, j))
        value = value * free(k, j)
        R0[tile(k, j), :] = value
        pre = value * INV[tile(k, j), :]
        V[0, tile(k, j), :] = pre
        return value * pre

    moments = [product_sum(first)]

    kroll = [ct[16 + 8 * s : 24 + 8 * s, :] for s in range(8)]

    def eight(v):
        e = [v[n] + v[7 - n] for n in range(4)]
        o = [v[n] - v[7 - n] for n in range(4)]
        out = [None] * 8
        for n in range(4):
            a, b = None, None
            for c in range(4):
                ta, tb = e[c] * float(KE[n, c]), o[c] * float(KO[n, c])
                a = ta if a is None else a + ta
                b = tb if b is None else b + tb
            out[n], out[7 - n] = a + b, a - b
        return out

    def local_operator(src, dst):
        for j in range(8):
            v = [src[tile(k, j), :] for k in range(8)]
            z = eight(v)
            for k in range(8):
                dst[tile(k, j), :] = z[k] * g2 + v[k] * g3
        energy = None
        for k in range(8):
            v = [src[tile(k, j), :] for j in range(8)]
            y = eight(v)
            for j in range(8):
                x = v[j] * kroll[0]
                for s in range(1, 8):
                    x = x + pltpu.roll(v[j], 8 - s, axis=0) * kroll[s]
                value = (dst[tile(k, j), :] + y[j] * g1 + x * g0) * (wcol * wkj(k, j))
                dst[tile(k, j), :] = value
                t = v[j] * value
                energy = t if energy is None else energy + t
        return energy

    def fold(n):
        def make(k, j):
            value = assembled(OUT, n + 1, k, j) * free(k, j)
            WA[n, tile(k, j), :] = value
            pre = value * INV[tile(k, j), :]
            if n < 2:
                V[n + 1, tile(k, j), :] = pre
            return value * pre

        return product_sum(make)

    for n in range(3):
        moments.append(local_operator(V.at[n], OUT))
        if n == 2:
            row = jnp.zeros((1, 128), F32)
            one = lax.broadcasted_iota(jnp.int32, (1, 128), 1)
            for at, t in enumerate(moments):
                t = jnp.sum(jnp.sum(t, axis=0, keepdims=True), axis=1, keepdims=True)
                row = jnp.where(one == at, t, row)
            ar[q] = row

            def tell(d, c):
                peer = lax.rem(q + d, NQ)
                pltpu.make_async_remote_copy(
                    ar.at[q], ar.at[q], ar_s.at[d], ar_r.at[q],
                    device_id=(m, peer), device_id_type=MESH).start()
                return c

            lax.fori_loop(1, NQ, tell, 0)
        sum_xy(OUT, 0, 8)
        for d in (-1, 1):
            when_there(d, lambda d=d: halo_copy(OUT, n + 1, d).start())
        if n < 2:
            evaluate(3 + n, 0, NB, 8)
            send_field(3 + n)
        wait_halo(OUT, n + 1)
        if n < 2:
            for d in (-1, 1):
                when_there(d, lambda d=d: halo_copy(OUT, n + 1, d).wait_send())
            moments.append(fold(n))
        else:
            fold(n)

    for f in range(1, 5):
        for s in range(5):
            when_there(s - 2, lambda f=f, s=s: ans_copy(f, s).wait_recv())
    for f in range(5):
        t = ans[0, f] + ans[1, f] + ans[2, f] + ans[3, f] + ans[4, f]
        for b in range(16):
            iv[f : f + 1, b * 128 : (b + 1) * 128] = t[b : b + 1, :]

    def hear(d, c):
        peer = lax.rem(q + d, NQ)
        pltpu.make_async_remote_copy(
            ar.at[peer], ar.at[peer], ar_s.at[d], ar_r.at[peer],
            device_id=(m, peer), device_id_type=MESH).wait_recv()
        return c

    lax.fori_loop(1, NQ, hear, 0)
    parts = [ar[n] for n in range(NQ)]
    while len(parts) > 1:
        parts = [parts[n] + parts[n + 1] for n in range(0, len(parts), 2)]
    sums = jnp.broadcast_to(parts[0], (8, 128))
    mu = [
        jnp.take_along_axis(sums, jnp.full((8, 128), n, jnp.int32), axis=1,
                            mode="promise_in_bounds")
        for n in range(6)
    ]

    def quad(c, shift):
        total = None
        for a in range(len(c)):
            for b in range(a, len(c)):
                t = c[a] * c[b] * mu[a + b + shift]
                t = t if a == b else t + t
                total = t if total is None else total + t
        return total

    one = jnp.ones((8, 128), F32)
    zero = jnp.zeros((8, 128), F32)
    rho, pi = [one], [one]
    xs = [zero, zero, zero]
    norm = mu[0]
    for n in range(3):
        alpha = norm / quad(pi, 1)
        for a in range(n + 1):
            xs[a] = xs[a] + alpha * pi[a]
        moved = [zero] + [alpha * c for c in pi]
        rho = [(rho[a] if a < len(rho) else zero) - moved[a] for a in range(n + 2)]
        if n < 2:
            new = quad(rho, 0)
            beta = new / norm
            pi = [rho[a] + (beta * pi[a] if a < len(pi) else zero) for a in range(n + 2)]
            norm = new

    on_plane = 1.0 - pm
    for k in range(8):
        for j in range(8):
            t = tile(k, j)
            vel[t, :] = (rows(QB, 64 + k * 8 + j) * on_plane + xs[0] * V[0, t, :]
                         + xs[1] * V[1, t, :] + xs[2] * V[2, t, :])
            res[t, :] = (R0[t, :] + rho[1] * WA[0, t, :] + rho[2] * WA[1, t, :]
                         + rho[3] * WA[2, t, :])

    for d in range(-2, 3):
        when_there(d, lambda d=d: req_copy(d).wait_send())
    for d in (-1, 1):
        when_there(d, lambda d=d: aux_copy(d).wait_send())
        when_there(d, lambda d=d: face_copy(d).wait_send())
        when_there(d, lambda d=d: halo_copy(FB, 0, d).wait_send())
        when_there(d, lambda d=d: halo_copy(OUT, 3, d).wait_send())
    for f in range(5):
        for s in range(5):
            when_there(2 - s, lambda f=f, s=s: ans_copy(f, s).wait_send())

    def left(d, c):
        peer = lax.rem(q + d, NQ)
        pltpu.make_async_remote_copy(
            ar.at[q], ar.at[q], ar_s.at[d], ar_r.at[q],
            device_id=(m, peer), device_id_type=MESH).wait_send()
        return c

    lax.fori_loop(1, NQ, left, 0)


def body(donor_fields, interp_weights, donor_owner, donor_element, geometry, wall_flag, forcing):
    vm = pl.BlockSpec(memory_space=pltpu.VMEM)
    hbm = pl.BlockSpec(memory_space=pl.ANY)
    dma = pltpu.SemaphoreType.DMA
    f32 = lambda *shape: pltpu.VMEM(shape, F32)
    return pl.pallas_call(
        kernel,
        out_shape=(
            jax.ShapeDtypeStruct((512, 128), F32),
            jax.ShapeDtypeStruct((512, 128), F32),
            jax.ShapeDtypeStruct((5, 2048), F32),
        ),
        in_specs=[hbm, vm, vm, vm, vm, vm, hbm, vm],
        out_specs=(vm, vm, vm),
        scratch_shapes=[
            f32(5, 512, 128), f32(512, 128), f32(64, 128), f32(5, 64, 128),
            f32(8, 128), f32(2, 8, 128), f32(24 * NB, 128), pltpu.VMEM((NB, 128), jnp.int32),
            f32(5, NB, 128), f32(5, 5, 16, 128),
            f32(512, 128), f32(512, 128), f32(512, 128), f32(512, 128),
            f32(3, 512, 128), f32(3, 512, 128), f32(512, 128), f32(128, 128), f32(128, 128),
            f32(2, 8, 128), f32(2, 8, 128), f32(4, 2, 64, 128), f32(NQ, 1, 128),
            dma((2,)), dma((5,)), dma((5,)), dma((2,)), dma((2,)), dma((5, 5)), dma((5, 5)),
            dma((2,)), dma((2,)), dma((4, 2)), dma((4, 2)), dma((NQ,)), dma((NQ,)),
        ],
        compiler_params=pltpu.CompilerParams(
            collective_id=0, has_side_effects=True, vmem_limit_bytes=32 * 1024 * 1024),
        name="step_window",
    )(
        donor_fields, interp_weights, donor_owner.reshape(16, 128),
        donor_element.reshape(16, 128), geometry, wall_flag, forcing,
        jnp.asarray(const_table()),
    )


def solution(mesh):
    both = ("mesh", "dom")
    in_specs = (
        P(None, None, both), P(None, None, both), P(both, None), P(both),
        P(None, both), P(None, both), P(None, both),
    )
    out_specs = (P(None, both), P(None, both), P(None, both))
    return jax.shard_map(body, mesh=mesh, in_specs=in_specs, out_specs=out_specs, check_vma=False)
```

```python
import functools

import jax
import jax.numpy as jnp
import numpy as np
from jax import lax
from jax.experimental import pallas as pl
from jax.experimental.pallas import tpu as pltpu
from jax.sharding import PartitionSpec as P

MESH = pl.DeviceIdType.MESH
F32 = jnp.float32
NQ = 64
NB = 80
KM = 6
HALF = KM * 64
BF16 = jnp.bfloat16


def legendre_pair(values, degree):
    previous = values * 0.0 + 1.0
    current = values * 1.0
    for order in range(2, degree + 1):
        previous, current = (
            current,
            ((2 * order - 1) * values * current - (order - 1) * previous) / order,
        )
    return current, previous


def gll():
    degree, count = 7, 8
    x = np.cos(np.pi * np.arange(count) / degree)
    for _ in range(80):
        top, lower = legendre_pair(x, degree)
        x = x - (x * top - lower) / (count * top)
    x = np.sort(x)
    top, _ = legendre_pair(x, degree)
    w = 2.0 / (degree * count * top * top)
    eye = np.eye(count)
    d = top[:, None] / (top[None, :] * (x[:, None] - x[None, :] + eye)) * (1.0 - eye)
    d[0, 0] = -degree * count / 4.0
    d[7, 7] = degree * count / 4.0
    return x, w, d


X, WQ, D = gll()
KP = (D.T * WQ[None, :]) @ D / WQ[:, None]
KP = 0.5 * (KP + KP[::-1, ::-1])
KE = 0.5 * (KP[:4, :4] + KP[:4, 7:3:-1])
KO = 0.5 * (KP[:4, :4] - KP[:4, 7:3:-1])
LC = np.array([1.0 / np.prod([X[n] - X[m] for m in range(8) if m != n]) for n in range(8)])


def const_table():
    lane = np.arange(128)
    xl = lane % 8
    rows = []
    rows.append(np.repeat(X[:, None], 128, 1))
    rows.append(np.repeat(WQ[:, None], 128, 1))
    for s in range(8):
        rows.append(np.repeat(np.array([KP[i, (i + s) % 8] for i in range(8)])[:, None], 128, 1))
    kx = np.zeros((8, 128))
    for i in range(8):
        kx[i] = np.where(xl == 0, KP[i, 0], np.where(xl == 7, KP[i, 7], 0.0))
    kx[0] = np.where(xl == 1, KP[7, 0], kx[0])
    kx[7] = np.where(xl == 6, KP[0, 7], kx[7])
    rows.append(kx)
    rows.append((np.arange(8)[:, None] == xl[None, :]).astype(float))
    return np.concatenate(rows, 0).astype(np.float32)


def kernel(
    donor_hbm, wts_hbm, owner_hbm, elem_hbm, geo_hbm, wall_hbm, forc_hbm, ct_hbm,
    vel, res, iv,
    donor, wts, owner, elem, geo, wall, forc, ct, nat, req_src, req, aux_src, aux, W, IDX, OH, DB,
    ans_src, ans, fbuf, nbf, got,
    FB, OUT, R0, INV, V, WA, DG, ND, QB, halo, ar,
    in_sem, req_s, req_r, aux_s, aux_r, ans_s, ans_r, nb_s, nb_r, halo_s, halo_r, ar_s, ar_r,
):
    m = lax.axis_index("mesh")
    q = lax.axis_index("dom")
    om = 1 - m
    barrier = pltpu.get_barrier_semaphore()

    def there(d):
        return jnp.logical_and(q + d >= 0, q + d < NQ)

    pairs = ((wts_hbm, wts), (ct_hbm, ct), (owner_hbm, owner), (elem_hbm, elem), (geo_hbm, geo),
             (wall_hbm, wall), (forc_hbm, forc), (donor_hbm, donor))
    loads = [pltpu.make_async_copy(a, b, in_sem.at[n]) for n, (a, b) in enumerate(pairs)]
    for load in loads:
        load.start()

    for d, s in ((-1, 0), (1, 1)):
        @pl.when(jnp.logical_not(there(d)))
        def _(s=s):
            aux[s] = jnp.zeros((8, 128), F32)
            for r in range(4):
                halo[r, s] = jnp.zeros((64, 128), F32)
    for d in (-2, -1, 1, 2):
        @pl.when(jnp.logical_not(there(d)))
        def _(d=d):
            req[2 - d] = jnp.zeros((64, 128), F32)
            ans[2 + d] = jnp.zeros((5, 16, 128), F32)

    def hears(side, s):
        r = 2 * side - 1
        return jnp.logical_and(there(r), there(r + s - 2))

    for side in range(2):
        for s in range(5):
            @pl.when(jnp.logical_not(hears(side, s)))
            def _(side=side, s=s):
                nbf[side, s] = jnp.zeros((2, 1, 128), F32)

    def greet(d, c):
        peer = lax.rem(q + d, NQ)
        pl.semaphore_signal(barrier, inc=1, device_id=(m, peer), device_id_type=MESH)
        return c

    lax.fori_loop(1, NQ, greet, 0, unroll=9)
    for d in range(-3, 4):
        @pl.when(there(d))
        def _(d=d):
            pl.semaphore_signal(barrier, inc=1, device_id=(om, q + d), device_id_type=MESH)

    i0 = lax.broadcasted_iota(jnp.int32, (8, 128), 0)
    lane = lax.broadcasted_iota(jnp.int32, (8, 128), 1)
    xl = lane & 7
    yl = lane >> 3
    for load in loads[:6]:
        load.wait()
    xcol = ct[0:8, :]
    wcol = ct[8:16, :]

    for d in range(3):
        for b in range(16):
            t = wts[d, :, b * 128 : (b + 1) * 128] * xcol
            nat[d * 16 + b : d * 16 + b + 1, :] = jnp.sum(t, axis=0, keepdims=True)
    nat[48:64, :] = (owner[...] * 128 + elem[...]).astype(F32)

    def lanes(value, at):
        return jnp.take_along_axis(value, at, axis=1, mode="promise_in_bounds")

    from_y = lane >> 4 == i0
    for d in range(4):
        for s in range(2):
            a = nat[d * 16 + s * 8 : d * 16 + s * 8 + 8, :]
            for k in range(8):
                t = lanes(a, ((lane >> 3) & 1) * 64 + k * 8 + (lane & 7))
                at = d * 16 + k * 2 + s
                req_src[at : at + 1, :] = jnp.sum(
                    jnp.where(from_y, t, 0.0), axis=0, keepdims=True)
    aux_src[0:4, :] = geo[...]
    aux_src[4:6, :] = jnp.dot(
        wall[...].astype(F32), ct[88:96, :], preferred_element_type=F32
    )
    aux_src[6:8, :] = jnp.zeros((2, 128), F32)

    def req_copy(d):
        return pltpu.make_async_remote_copy(
            req_src, req.at[d + 2], req_s.at[d + 2], req_r.at[d + 2],
            device_id=(om, q + d), device_id_type=MESH)

    def aux_copy(d):
        s = (d + 1) // 2
        return pltpu.make_async_remote_copy(
            aux_src, aux.at[1 - s], aux_s.at[s], aux_r.at[1 - s],
            device_id=(m, q + d), device_id_type=MESH)

    def halo_copy(src, r, d):
        s = (d + 1) // 2
        return pltpu.make_async_remote_copy(
            src.at[pl.ds(s * 448, 64)], halo.at[r, 1 - s], halo_s.at[r, s], halo_r.at[r, 1 - s],
            device_id=(m, q + d), device_id_type=MESH)

    def near_copy(s, side):
        return pltpu.make_async_remote_copy(
            fbuf.at[s, side], nbf.at[1 - side, s], nb_s.at[s, side], nb_r.at[1 - side, s],
            device_id=(om, q + 1 - s + 2 * side), device_id_type=MESH)

    def tells(s, side):
        return jnp.logical_and(there(2 - s), there(1 - s + 2 * side))

    def ans_copy(f, s):
        d = 2 - s
        at = s * 16 if isinstance(s, int) else pl.multiple_of(s * 16, 16)
        return pltpu.make_async_remote_copy(
            ans_src.at[f, pl.ds(at, 16)], ans.at[s, f], ans_s.at[f, s], ans_r.at[f, s],
            device_id=(om, q + d), device_id_type=MESH)

    def when_there(d, act):
        @pl.when(there(d))
        def _():
            act()

    m7x = jnp.logical_and(i0 == 7, xl < 7)
    m0x = jnp.logical_and(i0 == 0, xl > 0)
    m7y = jnp.logical_and(i0 == 7, yl < 15)
    m0y = jnp.logical_and(i0 == 0, yl > 0)
    xhi, xlo = xl < 7, xl > 0
    yhi, ylo = yl < 15, yl > 0

    def sum_xy(ref, base, planes):
        for k in range(planes):
            lo = ref[pl.ds(base + k * 64, 8, stride=8), :]
            hi = ref[pl.ds(base + k * 64 + 7, 8, stride=8), :]
            ref[pl.ds(base + k * 64, 8, stride=8), :] = lo + jnp.where(
                xlo, pltpu.roll(hi, 1, axis=1), 0.0)
            ref[pl.ds(base + k * 64 + 7, 8, stride=8), :] = hi + jnp.where(
                xhi, pltpu.roll(lo, 127, axis=1), 0.0)
        for k in range(planes):
            at = base + k * 64
            lo = ref[at : at + 8, :]
            hi = ref[at + 56 : at + 64, :]
            ref[at : at + 8, :] = lo + jnp.where(ylo, pltpu.roll(hi, 8, axis=1), 0.0)
            ref[at + 56 : at + 64, :] = hi + jnp.where(yhi, pltpu.roll(lo, 120, axis=1), 0.0)

    def rows(ref, n):
        return jnp.broadcast_to(ref[n : n + 1, :], (8, 128))

    g0, g1, g2, g3 = (rows(geo, n) for n in range(4))

    def tile(k, j):
        at = (k * 8 + j) * 8
        return slice(at, at + 8)

    def wkj(k, j):
        return float(WQ[k] * WQ[j])

    loads[6].wait()
    g3w = g3 * wcol
    for k in range(8):
        for j in range(8):
            FB[tile(k, j), :] = forc[tile(k, j), :] * (g3w * wkj(k, j))
    sum_xy(FB, 0, 8)

    kdiag = ct[16:24, :]

    def diag_tile(h0, h1, h2, h3, k, j):
        return (h0 * kdiag + h1 * float(KP[j, j]) + h2 * float(KP[k, k]) + h3) * (
            wcol * wkj(k, j))

    for k in range(8):
        for j in range(8):
            DG[tile(k, j), :] = diag_tile(g0, g1, g2, g3, k, j)
    sum_xy(DG, 0, 8)

    loads[7].wait()
    for f in range(5):
        for at in range(0, HALF, 64):
            value = donor[f, at : at + 64, :]
            high = value.astype(BF16)
            DB[f * HALF + at : f * HALF + at + 64, 0:128] = high
            DB[f * HALF + at : f * HALF + at + 64, 128:256] = (
                value - high.astype(F32)).astype(BF16)

    width = sum(there(d).astype(jnp.int32) for d in range(-3, 4))
    pl.semaphore_wait(barrier, NQ - 1 + width)
    for d in (2, -2, 1, -1, 0):
        when_there(d, lambda d=d: req_copy(d).start())
    for d in (-1, 1):
        when_there(d, lambda d=d: aux_copy(d).start())
    for d in (-1, 1):
        when_there(d, lambda d=d: halo_copy(FB, 0, d).start())
    for d, s in ((-1, 0), (1, 1)):
        when_there(d, lambda d=d, s=s: aux_copy(-d).wait_recv())

    plane = jnp.logical_or(
        jnp.logical_and(i0 == 0, xl == 0), jnp.logical_and(i0 == 7, xl == 7))
    pm = jnp.where(plane, 0.0, 1.0)

    def wall_count(row):
        return (row + jnp.where(m7x, pltpu.roll(row, 127, axis=1), 0.0)
                + jnp.where(m0x, pltpu.roll(row, 1, axis=1), 0.0))

    masks = {}
    for n, (j, edge) in enumerate(((0, yl == 0), (7, yl == 15))):
        own = wall_count(rows(aux_src, 4 + n))
        below = wall_count(jnp.broadcast_to(aux[0, 4 + n : 5 + n, :], (8, 128)))
        above = wall_count(jnp.broadcast_to(aux[1, 4 + n : 5 + n, :], (8, 128)))
        for name, count in (("lo", own + below), ("in", own), ("hi", own + above)):
            masks[j, name] = pm * (1.0 - jnp.where(edge, jnp.minimum(count, 1.0), 0.0))

    def free(k, j):
        if j not in (0, 7):
            return pm
        return masks[j, "lo" if k == 0 else "hi" if k == 7 else "in"]

    for s in range(2):
        h = [jnp.broadcast_to(aux[s, n : n + 1, :], (8, 128)) for n in range(4)]
        for j in range(8):
            ND[s * 64 + j * 8 : s * 64 + j * 8 + 8, :] = diag_tile(*h, 0, j)
    sum_xy(ND, 0, 2)
    for k in range(8):
        for j in range(8):
            value = DG[tile(k, j), :]
            if k == 0:
                value = value + ND[tile(0, j), :]
            if k == 7:
                value = value + ND[tile(1, j), :]
            INV[tile(k, j), :] = free(k, j) / value

    row_of = lax.broadcasted_iota(jnp.int32, (128, 128), 0)

    def weights(s):
        for h in range(2):
            at = s * 16 + 8 * h
            code = req[s, 48 + 8 * h : 56 + 8 * h, :] - (q * 128).astype(F32)
            mine = jnp.logical_and(code >= 0.0, code < 128.0)
            IDX[pl.ds(pl.multiple_of(at, 8), 8), :] = jnp.where(mine, code, 0.0).astype(jnp.int32)
            keep = jnp.where(mine, 1.0, 0.0)
            for d in range(3):
                xi = req[s, d * 16 + 8 * h : d * 16 + 8 * h + 8, :]
                t = [xi - float(X[n]) for n in range(8)]
                pre, suf = [None], [None] * 8
                for n in range(1, 8):
                    pre.append(t[n - 1] if n == 1 else pre[-1] * t[n - 1])
                for n in range(6, -1, -1):
                    suf[n] = t[7] if n == 6 else suf[n + 1] * t[n + 1]
                for n in range(8):
                    a = suf[0] if n == 0 else pre[7] if n == 7 else pre[n] * suf[n]
                    a = a * float(LC[n])
                    if d == 0:
                        a = a * keep
                    W[pl.ds(pl.multiple_of((s * 24 + d * 8 + n) * 16 + 8 * h, 8), 8), :] = a
        for u in range(16):
            column = jnp.broadcast_to(IDX[pl.ds(s * 16 + u, 1), :], (128, 128))
            OH[s, :, u * 128 : (u + 1) * 128] = jnp.where(
                row_of == column, 1.0, 0.0).astype(BF16)

    def evaluate(fields, s):
        hot = OH[s]
        hot = jnp.concatenate([hot, hot], axis=0)
        picked = {}
        for f in fields:
            picked[f] = jnp.dot(DB[f * HALF : (f + 1) * HALF, :], hot, preferred_element_type=F32)
        base = s * 384
        for f in fields:
            for u in range(16):
                idx = jnp.broadcast_to(IDX[pl.ds(s * 16 + u, 1), :], (8, 128))
                wi = W[pl.ds(base + u, 8, stride=16), :]
                wj = [jnp.broadcast_to(W[pl.ds(base + (8 + j) * 16 + u, 1), :], (8, 128))
                      for j in range(8)]
                total = None
                for k in range(8):
                    wk = jnp.broadcast_to(W[pl.ds(base + (16 + k) * 16 + u, 1), :], (8, 128))
                    part = None
                    for j in range(8):
                        t = tile(k, j)
                        if k < KM:
                            g = picked[f][t, u * 128 : (u + 1) * 128]
                        else:
                            g = lanes(donor[f, t, :], idx)
                        part = g * wj[j] if part is None else part + g * wj[j]
                    total = part * wk if total is None else total + part * wk
                line = jnp.sum(total * wi, axis=0, keepdims=True)
                ans_src[f, pl.ds(s * 16 + u, 1), :] = line
                if f == 0 and u in (0, 1, 14, 15):
                    fbuf[s, u // 14, u % 2] = line

    def all_slots(fields):
        def step(s, c):
            evaluate(fields, s)
            return c

        lax.fori_loop(0, 5, step, 0)
        for f in fields:
            for s in (0, 4, 1, 3, 2):
                when_there(2 - s, lambda f=f, s=s: ans_copy(f, s).start())

    def serve(n, c):
        s = 2 + ((n + 1) // 2) * (1 - 2 * (n % 2))
        when_there(2 - s, lambda: req_copy(s - 2).wait_recv())
        weights(s)
        evaluate((0,), s)
        when_there(2 - s, lambda: ans_copy(0, s).start())
        for side in range(2):
            @pl.when(tells(s, side))
            def _(side=side):
                near_copy(s, side).start()
        return c

    lax.fori_loop(0, 5, serve, 0)
    all_slots((1, 2))

    for s in range(5):
        when_there(s - 2, lambda s=s: ans_copy(0, s).wait_recv())
    for side in range(2):
        for s in range(5):
            @pl.when(hears(side, s))
            def _(side=side, s=s):
                near_copy(s, 1 - side).wait_recv()
    got[...] = ans[0, 0] + ans[1, 0] + ans[2, 0] + ans[3, 0] + ans[4, 0]

    def on_planes(low, high):
        at = yl * 8 + i0
        t = jnp.where(xl == 0, lanes(jnp.broadcast_to(low, (8, 128)), at),
                      jnp.where(xl == 7, lanes(jnp.broadcast_to(high, (8, 128)), at), 0.0))
        return (t + jnp.where(m7y, pltpu.roll(pltpu.roll(t, 120, axis=1), 7, axis=0), 0.0)
                + jnp.where(m0y, pltpu.roll(pltpu.roll(t, 8, axis=1), 1, axis=0), 0.0))

    T = [on_planes(got[2 * k : 2 * k + 1, :], got[2 * k + 1 : 2 * k + 2, :]) for k in range(8)]
    for side, k in ((0, 0), (1, 7)):
        low, high = (sum(nbf[side, s, n] for s in range(1, 5)) + nbf[side, 0, n]
                     for n in range(2))
        T[k] = T[k] + on_planes(low, high)
    czd = jnp.where(q > 0, 0.5, 1.0).astype(F32)
    czu = jnp.where(q < NQ - 1, 0.5, 1.0).astype(F32)
    cyv = jnp.where(jnp.logical_or(m7y, m0y), 0.5, 1.0)

    def spread_y(row):
        return (row + jnp.where(m7y, pltpu.roll(row, 120, axis=1), 0.0)
                + jnp.where(m0y, pltpu.roll(row, 8, axis=1), 0.0))

    gy = spread_y(g0)
    gy_below = spread_y(jnp.broadcast_to(aux[0, 0:1, :], (8, 128)))
    gy_above = spread_y(jnp.broadcast_to(aux[1, 0:1, :], (8, 128)))
    for k in range(8):
        b = T[k] * cyv
        gs = gy
        if k == 0:
            b, gs = b * czd, gs + gy_below
        if k == 7:
            b, gs = b * czu, gs + gy_above
        QB[64 + k * 8 : 72 + k * 8, :] = b
        t = b * gs
        t = jnp.where(xl == 1, pltpu.roll(t, 1, axis=1),
                      jnp.where(xl == 6, pltpu.roll(t, 127, axis=1), t))
        QB[k * 8 : k * 8 + 8, :] = t

    cx = jnp.where(jnp.logical_or(m7x, m0x), 0.5, 1.0)
    cxy = {0: cx * jnp.where(ylo, 0.5, 1.0), 7: cx * jnp.where(yhi, 0.5, 1.0)}

    def assembled(src, r, k, j):
        value = src[tile(k, j), :]
        if k == 0:
            value = value + halo[r, 0, j * 8 : j * 8 + 8, :]
        if k == 7:
            value = value + halo[r, 1, j * 8 : j * 8 + 8, :]
        return value

    def wait_halo(src, r):
        for d in (-1, 1):
            when_there(d, lambda d=d: halo_copy(src, r, -d).wait_recv())

    def product_sum(make):
        total = None
        for k in range(8):
            part = None
            for j in range(8):
                t = make(k, j) * cxy.get(j, cx)
                part = t if part is None else part + t
            if k == 0:
                part = part * czd
            if k == 7:
                part = part * czu
            total = part if total is None else total + part
        return total

    kxw = ct[80:88, :] * wcol
    wait_halo(FB, 0)

    def first(k, j):
        value = assembled(FB, 0, k, j) - rows(QB, k * 8 + j) * (kxw * wkj(k, j))
        value = value * free(k, j)
        R0[tile(k, j), :] = value
        pre = value * INV[tile(k, j), :]
        V[0, tile(k, j), :] = pre
        return value * pre

    moments = [product_sum(first)]

    kroll = [ct[16 + 8 * s : 24 + 8 * s, :] for s in range(8)]

    def eight(v):
        e = [v[n] + v[7 - n] for n in range(4)]
        o = [v[n] - v[7 - n] for n in range(4)]
        out = [None] * 8
        for n in range(4):
            a, b = None, None
            for c in range(4):
                ta, tb = e[c] * float(KE[n, c]), o[c] * float(KO[n, c])
                a = ta if a is None else a + ta
                b = tb if b is None else b + tb
            out[n], out[7 - n] = a + b, a - b
        return out

    def local_operator(src, dst):
        for j in range(8):
            v = [src[tile(k, j), :] for k in range(8)]
            z = eight(v)
            for k in range(8):
                dst[tile(k, j), :] = z[k] * g2 + v[k] * g3
        energy = None
        for k in range(8):
            v = [src[tile(k, j), :] for j in range(8)]
            y = eight(v)
            for j in range(8):
                x = v[j] * kroll[0]
                for s in range(1, 8):
                    x = x + pltpu.roll(v[j], 8 - s, axis=0) * kroll[s]
                value = (dst[tile(k, j), :] + y[j] * g1 + x * g0) * (wcol * wkj(k, j))
                dst[tile(k, j), :] = value
                t = v[j] * value
                energy = t if energy is None else energy + t
        return energy

    def fold(n):
        def make(k, j):
            value = assembled(OUT, n + 1, k, j) * free(k, j)
            WA[n, tile(k, j), :] = value
            pre = value * INV[tile(k, j), :]
            if n < 2:
                V[n + 1, tile(k, j), :] = pre
            return value * pre

        return product_sum(make)

    row = [jnp.zeros((1, 128), F32), 0]
    lane_of = lax.broadcasted_iota(jnp.int32, (1, 128), 1)

    def collect():
        while row[1] < len(moments):
            t = jnp.sum(jnp.sum(moments[row[1]], axis=0, keepdims=True), axis=1, keepdims=True)
            row[0] = jnp.where(lane_of == row[1], t, row[0])
            row[1] += 1
        return row[0]

    for n in range(3):
        moments.append(local_operator(V.at[n], OUT))
        if n == 2:
            ar[q] = collect()

            def tell(d, c):
                peer = lax.rem(q + d, NQ)
                pltpu.make_async_remote_copy(
                    ar.at[q], ar.at[q], ar_s.at[d], ar_r.at[q],
                    device_id=(m, peer), device_id_type=MESH).start()
                return c

            lax.fori_loop(1, NQ, tell, 0, unroll=9)
        sum_xy(OUT, 0, 8)
        for d in (-1, 1):
            when_there(d, lambda d=d: halo_copy(OUT, n + 1, d).start())
        if n < 2:
            collect()
            all_slots((3 + n,))
        wait_halo(OUT, n + 1)
        if n < 2:
            for d in (-1, 1):
                when_there(d, lambda d=d: halo_copy(OUT, n + 1, d).wait_send())
            moments.append(fold(n))
        else:
            fold(n)

    for f in range(1, 5):
        for s in range(5):
            when_there(s - 2, lambda f=f, s=s: ans_copy(f, s).wait_recv())
    from_k = (lane >> 3) & 7 == i0
    for f in range(5):
        for s in range(2):
            a = (ans[0, f, pl.ds(s, 8, stride=2), :] + ans[1, f, pl.ds(s, 8, stride=2), :]
                 + ans[2, f, pl.ds(s, 8, stride=2), :] + ans[3, f, pl.ds(s, 8, stride=2), :]
                 + ans[4, f, pl.ds(s, 8, stride=2), :])
            for y in range(8):
                t = lanes(a, y * 16 + (lane >> 6) * 8 + (lane & 7))
                at = (s * 8 + y) * 128
                iv[f : f + 1, at : at + 128] = jnp.sum(
                    jnp.where(from_k, t, 0.0), axis=0, keepdims=True)

    def hear(d, c):
        peer = lax.rem(q + d, NQ)
        pltpu.make_async_remote_copy(
            ar.at[peer], ar.at[peer], ar_s.at[d], ar_r.at[peer],
            device_id=(m, peer), device_id_type=MESH).wait_recv()
        return c

    lax.fori_loop(1, NQ, hear, 0, unroll=9)
    parts = [ar[n] for n in range(NQ)]
    while len(parts) > 1:
        parts = [parts[n] + parts[n + 1] for n in range(0, len(parts), 2)]
    sums = jnp.broadcast_to(parts[0], (8, 128))
    mu = [
        jnp.take_along_axis(sums, jnp.full((8, 128), n, jnp.int32), axis=1,
                            mode="promise_in_bounds")
        for n in range(6)
    ]

    def quad(c, shift):
        total = None
        for a in range(len(c)):
            for b in range(a, len(c)):
                t = c[a] * c[b] * mu[a + b + shift]
                t = t if a == b else t + t
                total = t if total is None else total + t
        return total

    one = jnp.ones((8, 128), F32)
    zero = jnp.zeros((8, 128), F32)
    rho, pi = [one], [one]
    xs = [zero, zero, zero]
    norm = mu[0]
    for n in range(3):
        alpha = norm / quad(pi, 1)
        for a in range(n + 1):
            xs[a] = xs[a] + alpha * pi[a]
        moved = [zero] + [alpha * c for c in pi]
        rho = [(rho[a] if a < len(rho) else zero) - moved[a] for a in range(n + 2)]
        if n < 2:
            new = quad(rho, 0)
            beta = new / norm
            pi = [rho[a] + (beta * pi[a] if a < len(pi) else zero) for a in range(n + 2)]
            norm = new

    on_plane = 1.0 - pm
    for k in range(8):
        for j in range(8):
            t = tile(k, j)
            vel[t, :] = (rows(QB, 64 + k * 8 + j) * on_plane + xs[0] * V[0, t, :]
                         + xs[1] * V[1, t, :] + xs[2] * V[2, t, :])
            res[t, :] = (R0[t, :] + rho[1] * WA[0, t, :] + rho[2] * WA[1, t, :]
                         + rho[3] * WA[2, t, :])

    for d in range(-2, 3):
        when_there(d, lambda d=d: req_copy(d).wait_send())
    for d in (-1, 1):
        when_there(d, lambda d=d: aux_copy(d).wait_send())
        when_there(d, lambda d=d: halo_copy(FB, 0, d).wait_send())
        when_there(d, lambda d=d: halo_copy(OUT, 3, d).wait_send())
    for f in range(5):
        for s in range(5):
            when_there(2 - s, lambda f=f, s=s: ans_copy(f, s).wait_send())

    for s in range(5):
        for side in range(2):
            @pl.when(tells(s, side))
            def _(s=s, side=side):
                near_copy(s, side).wait_send()

    def left(d, c):
        peer = lax.rem(q + d, NQ)
        pltpu.make_async_remote_copy(
            ar.at[q], ar.at[q], ar_s.at[d], ar_r.at[q],
            device_id=(m, peer), device_id_type=MESH).wait_send()
        return c

    lax.fori_loop(1, NQ, left, 0, unroll=9)


def write_out(vel, res, iv, vel_out, res_out, iv_out, sem):
    copies = [pltpu.make_async_copy(a, b, sem.at[n])
              for n, (a, b) in enumerate(((vel, vel_out), (res, res_out), (iv, iv_out)))]
    for copy in copies:
        copy.start()
    for copy in copies:
        copy.wait()


def body(donor_fields, interp_weights, donor_owner, donor_element, geometry, wall_flag, forcing):
    vm = pl.BlockSpec(memory_space=pltpu.VMEM)
    hbm = pl.BlockSpec(memory_space=pltpu.HBM)
    dma = pltpu.SemaphoreType.DMA
    f32 = lambda *shape: pltpu.VMEM(shape, F32)
    held = pl.pallas_call(
        kernel,
        out_shape=(
            jax.ShapeDtypeStruct((512, 128), F32),
            jax.ShapeDtypeStruct((512, 128), F32),
            jax.ShapeDtypeStruct((5, 2048), F32),
        ),
        in_specs=[hbm] * 8,
        out_specs=(vm, vm, vm),
        scratch_shapes=[
            f32(5, 512, 128), f32(3, 8, 2048), pltpu.VMEM((16, 128), jnp.int32),
            pltpu.VMEM((16, 128), jnp.int32), f32(4, 128), pltpu.VMEM((2, 8), jnp.int32),
            f32(512, 128), f32(96, 128), f32(64, 128), f32(64, 128), f32(5, 64, 128),
            f32(8, 128), f32(2, 8, 128), f32(24 * NB, 128), pltpu.VMEM((NB, 128), jnp.int32),
            pltpu.VMEM((5, 128, 2048), BF16), pltpu.VMEM((5 * HALF, 256), BF16),
            f32(5, NB, 128), f32(5, 5, 16, 128), f32(5, 2, 2, 1, 128), f32(2, 5, 2, 1, 128), f32(16, 128),
            f32(512, 128), f32(512, 128), f32(512, 128), f32(512, 128),
            f32(3, 512, 128), f32(3, 512, 128), f32(512, 128), f32(128, 128), f32(128, 128),
            f32(4, 2, 64, 128), f32(NQ, 1, 128),
            dma((8,)), dma((5,)), dma((5,)), dma((2,)), dma((2,)), dma((5, 5)), dma((5, 5)),
            dma((5, 2)), dma((2, 5)), dma((4, 2)), dma((4, 2)), dma((NQ,)), dma((NQ,)),
        ],
        compiler_params=pltpu.CompilerParams(
            collective_id=0, has_side_effects=True, vmem_limit_bytes=64500000),
        name="step_window",
    )(
        donor_fields, interp_weights, donor_owner.reshape(16, 128),
        donor_element.reshape(16, 128), geometry, wall_flag, forcing,
        jnp.asarray(const_table()),
    )
    return pl.pallas_call(
        write_out,
        out_shape=tuple(jax.ShapeDtypeStruct(a.shape, F32) for a in held),
        in_specs=[vm] * 3,
        out_specs=(hbm,) * 3,
        scratch_shapes=[dma((3,))],
        name="write_out",
    )(*held)


def solution(mesh):
    both = ("mesh", "dom")
    in_specs = (
        P(None, None, both), P(None, None, both), P(both, None), P(both),
        P(None, both), P(None, both), P(None, both),
    )
    out_specs = (P(None, both), P(None, both), P(None, both))
    return jax.shard_map(body, mesh=mesh, in_specs=in_specs, out_specs=out_specs, check_vma=False)
```

```python
import functools

import jax
import jax.numpy as jnp
import numpy as np
from jax import lax
from jax.experimental import pallas as pl
from jax.experimental.pallas import tpu as pltpu
from jax.sharding import PartitionSpec as P

MESH = pl.DeviceIdType.MESH
F32 = jnp.float32
NQ = 64
NB = 80
KM = 6
HALF = KM * 64
BF16 = jnp.bfloat16


def legendre_pair(values, degree):
    previous = values * 0.0 + 1.0
    current = values * 1.0
    for order in range(2, degree + 1):
        previous, current = (
            current,
            ((2 * order - 1) * values * current - (order - 1) * previous) / order,
        )
    return current, previous


def gll():
    degree, count = 7, 8
    x = np.cos(np.pi * np.arange(count) / degree)
    for _ in range(80):
        top, lower = legendre_pair(x, degree)
        x = x - (x * top - lower) / (count * top)
    x = np.sort(x)
    top, _ = legendre_pair(x, degree)
    w = 2.0 / (degree * count * top * top)
    eye = np.eye(count)
    d = top[:, None] / (top[None, :] * (x[:, None] - x[None, :] + eye)) * (1.0 - eye)
    d[0, 0] = -degree * count / 4.0
    d[7, 7] = degree * count / 4.0
    return x, w, d


X, WQ, D = gll()
KP = (D.T * WQ[None, :]) @ D / WQ[:, None]
KP = 0.5 * (KP + KP[::-1, ::-1])
KE = 0.5 * (KP[:4, :4] + KP[:4, 7:3:-1])
KO = 0.5 * (KP[:4, :4] - KP[:4, 7:3:-1])
LC = np.array([1.0 / np.prod([X[n] - X[m] for m in range(8) if m != n]) for n in range(8)])


def const_table():
    lane = np.arange(128)
    xl = lane % 8
    rows = []
    rows.append(np.repeat(X[:, None], 128, 1))
    rows.append(np.repeat(WQ[:, None], 128, 1))
    for s in range(8):
        rows.append(np.repeat(np.array([KP[i, (i + s) % 8] for i in range(8)])[:, None], 128, 1))
    kx = np.zeros((8, 128))
    for i in range(8):
        kx[i] = np.where(xl == 0, KP[i, 0], np.where(xl == 7, KP[i, 7], 0.0))
    kx[0] = np.where(xl == 1, KP[7, 0], kx[0])
    kx[7] = np.where(xl == 6, KP[0, 7], kx[7])
    rows.append(kx)
    rows.append((np.arange(8)[:, None] == xl[None, :]).astype(float))
    return np.concatenate(rows, 0).astype(np.float32)


def kernel(
    donor_hbm, wts_hbm, owner_hbm, elem_hbm, geo_hbm, wall_hbm, forc_hbm, ct_hbm,
    vel, res, iv,
    donor, wts, owner, elem, geo, wall, forc, ct, nat, req_src, req, aux_src, aux, W, IDX, OH, DB,
    ans_src, ans, fbuf, nbf, got,
    FB, OUT, INV, V, SB, DG, ND, QB, halo, ar,
    in_sem, req_s, req_r, aux_s, aux_r, ans_s, ans_r, nb_s, nb_r, halo_s, halo_r, ar_s, ar_r,
):
    m = lax.axis_index("mesh")
    q = lax.axis_index("dom")
    om = 1 - m
    barrier = pltpu.get_barrier_semaphore()

    def there(d):
        return jnp.logical_and(q + d >= 0, q + d < NQ)

    pairs = ((wts_hbm, wts), (ct_hbm, ct), (owner_hbm, owner), (elem_hbm, elem), (geo_hbm, geo),
             (wall_hbm, wall), (forc_hbm, forc), (donor_hbm, donor))
    loads = [pltpu.make_async_copy(a, b, in_sem.at[n]) for n, (a, b) in enumerate(pairs)]
    for load in loads:
        load.start()

    for d, s in ((-1, 0), (1, 1)):
        @pl.when(jnp.logical_not(there(d)))
        def _(s=s):
            aux[s] = jnp.zeros((8, 128), F32)
            for r in range(4):
                halo[r, s] = jnp.zeros((64, 128), F32)
    for d in (-2, -1, 1, 2):
        @pl.when(jnp.logical_not(there(d)))
        def _(d=d):
            req[2 - d] = jnp.zeros((64, 128), F32)
            ans[2 + d] = jnp.zeros((5, 16, 128), F32)

    def hears(side, s):
        r = 2 * side - 1
        return jnp.logical_and(there(r), there(r + s - 2))

    for side in range(2):
        for s in range(5):
            @pl.when(jnp.logical_not(hears(side, s)))
            def _(side=side, s=s):
                nbf[side, s] = jnp.zeros((2, 1, 128), F32)

    def greet(d, c):
        peer = lax.rem(q + d, NQ)
        pl.semaphore_signal(barrier, inc=1, device_id=(m, peer), device_id_type=MESH)
        return c

    lax.fori_loop(1, NQ, greet, 0, unroll=9)
    for d in range(-3, 4):
        @pl.when(there(d))
        def _(d=d):
            pl.semaphore_signal(barrier, inc=1, device_id=(om, q + d), device_id_type=MESH)

    i0 = lax.broadcasted_iota(jnp.int32, (8, 128), 0)
    lane = lax.broadcasted_iota(jnp.int32, (8, 128), 1)
    xl = lane & 7
    yl = lane >> 3
    for load in loads[:6]:
        load.wait()
    xcol = ct[0:8, :]
    wcol = ct[8:16, :]

    for d in range(3):
        for b in range(16):
            t = wts[d, :, b * 128 : (b + 1) * 128] * xcol
            nat[d * 16 + b : d * 16 + b + 1, :] = jnp.sum(t, axis=0, keepdims=True)
    nat[48:64, :] = (owner[...] * 128 + elem[...]).astype(F32)

    def lanes(value, at):
        return jnp.take_along_axis(value, at, axis=1, mode="promise_in_bounds")

    from_y = lane >> 4 == i0
    for d in range(4):
        for s in range(2):
            a = nat[d * 16 + s * 8 : d * 16 + s * 8 + 8, :]
            for k in range(8):
                t = lanes(a, ((lane >> 3) & 1) * 64 + k * 8 + (lane & 7))
                at = d * 16 + k * 2 + s
                req_src[at : at + 1, :] = jnp.sum(
                    jnp.where(from_y, t, 0.0), axis=0, keepdims=True)
    aux_src[0:4, :] = geo[...]
    aux_src[4:6, :] = jnp.dot(
        wall[...].astype(F32), ct[88:96, :], preferred_element_type=F32
    )
    aux_src[6:8, :] = jnp.zeros((2, 128), F32)

    def req_copy(d):
        return pltpu.make_async_remote_copy(
            req_src, req.at[d + 2], req_s.at[d + 2], req_r.at[d + 2],
            device_id=(om, q + d), device_id_type=MESH)

    def aux_copy(d):
        s = (d + 1) // 2
        return pltpu.make_async_remote_copy(
            aux_src, aux.at[1 - s], aux_s.at[s], aux_r.at[1 - s],
            device_id=(m, q + d), device_id_type=MESH)

    def halo_copy(src, r, d):
        s = (d + 1) // 2
        return pltpu.make_async_remote_copy(
            src.at[pl.ds(s * 448, 64)], halo.at[r, 1 - s], halo_s.at[r, s], halo_r.at[r, 1 - s],
            device_id=(m, q + d), device_id_type=MESH)

    def near_copy(s, side):
        return pltpu.make_async_remote_copy(
            fbuf.at[s, side], nbf.at[1 - side, s], nb_s.at[s, side], nb_r.at[1 - side, s],
            device_id=(om, q + 1 - s + 2 * side), device_id_type=MESH)

    def tells(s, side):
        return jnp.logical_and(there(2 - s), there(1 - s + 2 * side))

    def ans_copy(f, s):
        d = 2 - s
        at = s * 16 if isinstance(s, int) else pl.multiple_of(s * 16, 16)
        return pltpu.make_async_remote_copy(
            ans_src.at[f, pl.ds(at, 16)], ans.at[s, f], ans_s.at[f, s], ans_r.at[f, s],
            device_id=(om, q + d), device_id_type=MESH)

    def when_there(d, act):
        @pl.when(there(d))
        def _():
            act()

    m7x = jnp.logical_and(i0 == 7, xl < 7)
    m0x = jnp.logical_and(i0 == 0, xl > 0)
    m7y = jnp.logical_and(i0 == 7, yl < 15)
    m0y = jnp.logical_and(i0 == 0, yl > 0)
    xhi, xlo = xl < 7, xl > 0
    yhi, ylo = yl < 15, yl > 0

    def sum_xy(ref, base, planes):
        for k in range(planes):
            lo = ref[pl.ds(base + k * 64, 8, stride=8), :]
            hi = ref[pl.ds(base + k * 64 + 7, 8, stride=8), :]
            ref[pl.ds(base + k * 64, 8, stride=8), :] = lo + jnp.where(
                xlo, pltpu.roll(hi, 1, axis=1), 0.0)
            ref[pl.ds(base + k * 64 + 7, 8, stride=8), :] = hi + jnp.where(
                xhi, pltpu.roll(lo, 127, axis=1), 0.0)
        for k in range(planes):
            at = base + k * 64
            lo = ref[at : at + 8, :]
            hi = ref[at + 56 : at + 64, :]
            ref[at : at + 8, :] = lo + jnp.where(ylo, pltpu.roll(hi, 8, axis=1), 0.0)
            ref[at + 56 : at + 64, :] = hi + jnp.where(yhi, pltpu.roll(lo, 120, axis=1), 0.0)

    def rows(ref, n):
        return jnp.broadcast_to(ref[n : n + 1, :], (8, 128))

    g0, g1, g2, g3 = (rows(geo, n) for n in range(4))

    def tile(k, j):
        at = (k * 8 + j) * 8
        return slice(at, at + 8)

    def wkj(k, j):
        return float(WQ[k] * WQ[j])

    loads[7].wait()
    for f in range(1):
        for at in range(0, HALF, 64):
            value = donor[f, at : at + 64, :]
            high = value.astype(BF16)
            DB[f * HALF + at : f * HALF + at + 64, 0:128] = high
            DB[f * HALF + at : f * HALF + at + 64, 128:256] = (
                value - high.astype(F32)).astype(BF16)

    loads[6].wait()
    g3w = g3 * wcol
    for k in range(8):
        for j in range(8):
            FB[tile(k, j), :] = forc[tile(k, j), :] * (g3w * wkj(k, j))
    sum_xy(FB, 0, 8)

    width = sum(there(d).astype(jnp.int32) for d in range(-3, 4))
    pl.semaphore_wait(barrier, NQ - 1 + width)
    for d in (2, -2, 1, -1, 0):
        when_there(d, lambda d=d: req_copy(d).start())
    for d in (-1, 1):
        when_there(d, lambda d=d: aux_copy(d).start())
    kdiag = ct[16:24, :]

    def diag_tile(h0, h1, h2, h3, k, j):
        return (h0 * kdiag + h1 * float(KP[j, j]) + h2 * float(KP[k, k]) + h3) * (
            wcol * wkj(k, j))

    for k in range(8):
        for j in range(8):
            DG[tile(k, j), :] = diag_tile(g0, g1, g2, g3, k, j)
    sum_xy(DG, 0, 8)

    for f in range(1, 5):
        for at in range(0, HALF, 64):
            value = donor[f, at : at + 64, :]
            high = value.astype(BF16)
            DB[f * HALF + at : f * HALF + at + 64, 0:128] = high
            DB[f * HALF + at : f * HALF + at + 64, 128:256] = (
                value - high.astype(F32)).astype(BF16)

    plane = jnp.logical_or(
        jnp.logical_and(i0 == 0, xl == 0), jnp.logical_and(i0 == 7, xl == 7))
    pm = jnp.where(plane, 0.0, 1.0)

    def wall_count(row):
        return (row + jnp.where(m7x, pltpu.roll(row, 127, axis=1), 0.0)
                + jnp.where(m0x, pltpu.roll(row, 1, axis=1), 0.0))

    masks = {}
    edges = ((0, yl == 0), (7, yl == 15))

    def wall_mask(j, name, count):
        edge = edges[j // 7][1]
        masks[j, name] = pm * (1.0 - jnp.where(edge, jnp.minimum(count, 1.0), 0.0))

    own = [wall_count(rows(aux_src, 4 + n)) for n in range(2)]
    for n in range(2):
        wall_mask(7 * n, "in", own[n])

    def free(k, j):
        if j not in (0, 7):
            return pm
        return masks[j, "lo" if k == 0 else "hi" if k == 7 else "in"]

    for k in range(1, 7):
        for j in range(8):
            INV[tile(k, j), :] = free(k, j) / DG[tile(k, j), :]

    row_of = lax.broadcasted_iota(jnp.int32, (128, 128), 0)

    def weights(s):
        for h in range(2):
            at = s * 16 + 8 * h
            code = req[s, 48 + 8 * h : 56 + 8 * h, :] - (q * 128).astype(F32)
            mine = jnp.logical_and(code >= 0.0, code < 128.0)
            IDX[pl.ds(pl.multiple_of(at, 8), 8), :] = jnp.where(mine, code, 0.0).astype(jnp.int32)
            keep = jnp.where(mine, 1.0, 0.0)
            for d in range(3):
                xi = req[s, d * 16 + 8 * h : d * 16 + 8 * h + 8, :]
                t = [xi - float(X[n]) for n in range(8)]
                pre, suf = [None], [None] * 8
                for n in range(1, 8):
                    pre.append(t[n - 1] if n == 1 else pre[-1] * t[n - 1])
                for n in range(6, -1, -1):
                    suf[n] = t[7] if n == 6 else suf[n + 1] * t[n + 1]
                for n in range(8):
                    a = suf[0] if n == 0 else pre[7] if n == 7 else pre[n] * suf[n]
                    a = a * float(LC[n])
                    if d == 0:
                        a = a * keep
                    W[pl.ds(pl.multiple_of((s * 24 + d * 8 + n) * 16 + 8 * h, 8), 8), :] = a
        for u in range(16):
            column = jnp.broadcast_to(IDX[pl.ds(s * 16 + u, 1), :], (128, 128))
            OH[s, :, u * 128 : (u + 1) * 128] = jnp.where(
                row_of == column, 1.0, 0.0).astype(BF16)

    def evaluate(fields, s):
        hot = OH[s]
        hot = jnp.concatenate([hot, hot], axis=0)
        picked = {}
        for f in fields:
            picked[f] = jnp.dot(DB[f * HALF : (f + 1) * HALF, :], hot, preferred_element_type=F32)
        base = s * 384
        for f in fields:
            for u in range(16):
                idx = jnp.broadcast_to(IDX[pl.ds(s * 16 + u, 1), :], (8, 128))
                wi = W[pl.ds(base + u, 8, stride=16), :]
                wj = [jnp.broadcast_to(W[pl.ds(base + (8 + j) * 16 + u, 1), :], (8, 128))
                      for j in range(8)]
                total = None
                for k in range(8):
                    wk = jnp.broadcast_to(W[pl.ds(base + (16 + k) * 16 + u, 1), :], (8, 128))
                    part = None
                    for j in range(8):
                        t = tile(k, j)
                        if k < KM:
                            g = picked[f][t, u * 128 : (u + 1) * 128]
                        else:
                            g = lanes(donor[f, t, :], idx)
                        part = g * wj[j] if part is None else part + g * wj[j]
                    total = part * wk if total is None else total + part * wk
                line = jnp.sum(total * wi, axis=0, keepdims=True)
                ans_src[f, pl.ds(s * 16 + u, 1), :] = line
                if f == 0 and u in (0, 1, 14, 15):
                    fbuf[s, u // 14, u % 2] = line

    def all_slots(fields):
        def step(s, c):
            evaluate(fields, s)
            return c

        lax.fori_loop(0, 5, step, 0)
        for f in fields:
            for s in (0, 4, 1, 3, 2):
                when_there(2 - s, lambda f=f, s=s: ans_copy(f, s).start())

    def serve(n, c):
        s = 2 + ((n + 1) // 2) * (1 - 2 * (n % 2))
        when_there(2 - s, lambda: req_copy(s - 2).wait_recv())
        weights(s)
        evaluate((0,), s)
        when_there(2 - s, lambda: ans_copy(0, s).start())
        for side in range(2):
            @pl.when(tells(s, side))
            def _(side=side):
                near_copy(s, side).start()
        return c

    lax.fori_loop(0, 5, serve, 0)
    for d in (-1, 1):
        when_there(d, lambda d=d: halo_copy(FB, 0, d).start())
    for d, s in ((-1, 0), (1, 1)):
        when_there(d, lambda d=d, s=s: aux_copy(-d).wait_recv())

    for n in range(2):
        for s, name in ((0, "lo"), (1, "hi")):
            other = wall_count(jnp.broadcast_to(aux[s, 4 + n : 5 + n, :], (8, 128)))
            wall_mask(7 * n, name, own[n] + other)

    for s in range(2):
        h = [jnp.broadcast_to(aux[s, n : n + 1, :], (8, 128)) for n in range(4)]
        for j in range(8):
            ND[s * 64 + j * 8 : s * 64 + j * 8 + 8, :] = diag_tile(*h, 0, j)
    sum_xy(ND, 0, 2)
    for k in (0, 7):
        for j in range(8):
            value = DG[tile(k, j), :] + ND[tile(k // 7, j), :]
            INV[tile(k, j), :] = free(k, j) / value

    all_slots((1, 2))

    for s in range(5):
        when_there(s - 2, lambda s=s: ans_copy(0, s).wait_recv())
    for side in range(2):
        for s in range(5):
            @pl.when(hears(side, s))
            def _(side=side, s=s):
                near_copy(s, 1 - side).wait_recv()
    got[...] = ans[0, 0] + ans[1, 0] + ans[2, 0] + ans[3, 0] + ans[4, 0]

    def on_planes(low, high):
        at = yl * 8 + i0
        t = jnp.where(xl == 0, lanes(jnp.broadcast_to(low, (8, 128)), at),
                      jnp.where(xl == 7, lanes(jnp.broadcast_to(high, (8, 128)), at), 0.0))
        return (t + jnp.where(m7y, pltpu.roll(pltpu.roll(t, 120, axis=1), 7, axis=0), 0.0)
                + jnp.where(m0y, pltpu.roll(pltpu.roll(t, 8, axis=1), 1, axis=0), 0.0))

    T = [on_planes(got[2 * k : 2 * k + 1, :], got[2 * k + 1 : 2 * k + 2, :]) for k in range(8)]
    for side, k in ((0, 0), (1, 7)):
        low, high = (sum(nbf[side, s, n] for s in range(1, 5)) + nbf[side, 0, n]
                     for n in range(2))
        T[k] = T[k] + on_planes(low, high)
    czd = jnp.where(q > 0, 0.5, 1.0).astype(F32)
    czu = jnp.where(q < NQ - 1, 0.5, 1.0).astype(F32)
    cyv = jnp.where(jnp.logical_or(m7y, m0y), 0.5, 1.0)

    def spread_y(row):
        return (row + jnp.where(m7y, pltpu.roll(row, 120, axis=1), 0.0)
                + jnp.where(m0y, pltpu.roll(row, 8, axis=1), 0.0))

    gy = spread_y(g0)
    gy_below = spread_y(jnp.broadcast_to(aux[0, 0:1, :], (8, 128)))
    gy_above = spread_y(jnp.broadcast_to(aux[1, 0:1, :], (8, 128)))
    for k in range(8):
        b = T[k] * cyv
        gs = gy
        if k == 0:
            b, gs = b * czd, gs + gy_below
        if k == 7:
            b, gs = b * czu, gs + gy_above
        QB[64 + k * 8 : 72 + k * 8, :] = b
        t = b * gs
        t = jnp.where(xl == 1, pltpu.roll(t, 1, axis=1),
                      jnp.where(xl == 6, pltpu.roll(t, 127, axis=1), t))
        QB[k * 8 : k * 8 + 8, :] = t

    cx = jnp.where(jnp.logical_or(m7x, m0x), 0.5, 1.0)
    cxy = {0: cx * jnp.where(ylo, 0.5, 1.0), 7: cx * jnp.where(yhi, 0.5, 1.0)}

    def assembled(src, r, k, j):
        value = src[tile(k, j), :]
        if k == 0:
            value = value + halo[r, 0, j * 8 : j * 8 + 8, :]
        if k == 7:
            value = value + halo[r, 1, j * 8 : j * 8 + 8, :]
        return value

    def wait_halo(src, r):
        for d in (-1, 1):
            when_there(d, lambda d=d: halo_copy(src, r, -d).wait_recv())

    def inner_sums(make, count, planes=range(8)):
        totals = [None] * count
        for k in planes:
            parts = [None] * count
            for j in range(8):
                one, others = make(k, j)
                one = one * cxy.get(j, cx)
                for n, other in enumerate(others):
                    t = one * other
                    parts[n] = t if parts[n] is None else parts[n] + t
            for n in range(count):
                t = parts[n]
                if k == 0:
                    t = t * czd
                if k == 7:
                    t = t * czu
                totals[n] = t if totals[n] is None else totals[n] + t
        return totals

    kxw = ct[80:88, :] * wcol
    wait_halo(FB, 0)

    def first(k, j):
        value = assembled(FB, 0, k, j) - rows(QB, k * 8 + j) * (kxw * wkj(k, j))
        value = value * free(k, j)
        SB[0, tile(k, j), :] = value
        pre = value * INV[tile(k, j), :]
        V[0, tile(k, j), :] = pre
        return pre, (value,)

    moments = inner_sums(first, 1)

    kroll = [ct[16 + 8 * s : 24 + 8 * s, :] for s in range(8)]

    def eight(v):
        e = [v[n] + v[7 - n] for n in range(4)]
        o = [v[n] - v[7 - n] for n in range(4)]
        out = [None] * 8
        for n in range(4):
            a, b = None, None
            for c in range(4):
                ta, tb = e[c] * float(KE[n, c]), o[c] * float(KO[n, c])
                a = ta if a is None else a + ta
                b = tb if b is None else b + tb
            out[n], out[7 - n] = a + b, a - b
        return out

    def ends_of_eight(v):
        a, b = None, None
        for c in range(4):
            ta, tb = (v[c] + v[7 - c]) * float(KE[0, c]), (v[c] - v[7 - c]) * float(KO[0, c])
            a = ta if a is None else a + ta
            b = tb if b is None else b + tb
        return {0: a + b, 7: a - b}

    def local_operator(src, dst, planes, wanted):
        faces = len(planes) == 2
        for j in range(8):
            v = [src[tile(k, j), :] for k in range(8)]
            z = ends_of_eight(v) if faces else eight(v)
            for k in planes:
                dst[tile(k, j), :] = z[k] * g2 + v[k] * g3
        energy = None
        for k in planes:
            v = [src[tile(k, j), :] for j in range(8)]
            y = eight(v)
            for j in range(8):
                x = v[j] * kroll[0]
                for s in range(1, 8):
                    x = x + pltpu.roll(v[j], 8 - s, axis=0) * kroll[s]
                value = (dst[tile(k, j), :] + y[j] * g1 + x * g0) * (wcol * wkj(k, j))
                dst[tile(k, j), :] = value
                if wanted:
                    t = v[j] * value
                    energy = t if energy is None else energy + t
        return energy

    def fold(n, planes):
        def make(k, j):
            t = tile(k, j)
            value = assembled(OUT, n + 1, k, j) * free(k, j) - SB[n, t, :]
            SB[n + 1, t, :] = value
            pre = value * INV[t, :]
            V[n + 1, t, :] = pre
            return pre, tuple(SB[a, t, :] for a in range(n + 1)) + (value,)

        return inner_sums(make, n + 2, planes)

    row = [jnp.zeros((1, 128), F32), 0]
    lane_of = lax.broadcasted_iota(jnp.int32, (1, 128), 1)

    def collect():
        while row[1] < len(moments):
            t = jnp.sum(jnp.sum(moments[row[1]], axis=0, keepdims=True), axis=1, keepdims=True)
            row[0] = jnp.where(lane_of == row[1], t, row[0])
            row[1] += 1
        return row[0]

    for n in range(2):
        local_operator(V.at[n], OUT, (0, 7), False)
        sum_xy(OUT, 0, 1)
        sum_xy(OUT, 448, 1)
        for d in (-1, 1):
            when_there(d, lambda d=d: halo_copy(OUT, n + 1, d).start())
        local_operator(V.at[n], OUT, range(1, 7), False)
        sum_xy(OUT, 64, 6)
        inside = fold(n, range(1, 7))
        collect()
        all_slots((3 + n,))
        wait_halo(OUT, n + 1)
        for d in (-1, 1):
            when_there(d, lambda d=d: halo_copy(OUT, n + 1, d).wait_send())
        moments.extend(a + b for a, b in zip(inside, fold(n, (0, 7))))

    moments.append(local_operator(V.at[2], OUT, range(8), True))
    ar[q] = collect()

    def tell(d, c):
        peer = lax.rem(q + d, NQ)
        pltpu.make_async_remote_copy(
            ar.at[q], ar.at[q], ar_s.at[d], ar_r.at[q],
            device_id=(m, peer), device_id_type=MESH).start()
        return c

    lax.fori_loop(1, NQ, tell, 0, unroll=9)
    sum_xy(OUT, 0, 8)
    for d in (-1, 1):
        when_there(d, lambda d=d: halo_copy(OUT, 3, d).start())

    for f in range(1, 5):
        for s in range(5):
            when_there(s - 2, lambda f=f, s=s: ans_copy(f, s).wait_recv())
    from_k = (lane >> 3) & 7 == i0
    for f in range(5):
        for s in range(2):
            a = (ans[0, f, pl.ds(s, 8, stride=2), :] + ans[1, f, pl.ds(s, 8, stride=2), :]
                 + ans[2, f, pl.ds(s, 8, stride=2), :] + ans[3, f, pl.ds(s, 8, stride=2), :]
                 + ans[4, f, pl.ds(s, 8, stride=2), :])
            for y in range(8):
                t = lanes(a, y * 16 + (lane >> 6) * 8 + (lane & 7))
                at = (s * 8 + y) * 128
                iv[f : f + 1, at : at + 128] = jnp.sum(
                    jnp.where(from_k, t, 0.0), axis=0, keepdims=True)

    wait_halo(OUT, 3)

    def hear(d, c):
        peer = lax.rem(q + d, NQ)
        pltpu.make_async_remote_copy(
            ar.at[peer], ar.at[peer], ar_s.at[d], ar_r.at[peer],
            device_id=(m, peer), device_id_type=MESH).wait_recv()
        return c

    lax.fori_loop(1, NQ, hear, 0, unroll=9)
    parts = [ar[n] for n in range(NQ)]
    while len(parts) > 1:
        parts = [parts[n] + parts[n + 1] for n in range(0, len(parts), 2)]
    sums = jnp.broadcast_to(parts[0], (8, 128))
    mu = [
        jnp.take_along_axis(sums, jnp.full((8, 128), n, jnp.int32), axis=1,
                            mode="promise_in_bounds")
        for n in range(7)
    ]

    gram = {(0, 0): mu[0], (0, 1): mu[1], (1, 1): mu[2], (0, 2): mu[3], (1, 2): mu[4],
            (2, 2): mu[5]}
    stiff = {(0, 0): mu[1] + mu[0], (0, 1): mu[2] + mu[1], (1, 1): mu[4] + mu[2],
             (0, 2): mu[4] + mu[3], (1, 2): mu[5] + mu[4], (2, 2): mu[6]}

    def quad(c, form):
        total = None
        for a in range(len(c)):
            for b in range(a, len(c)):
                t = c[a] * c[b] * form[a, b]
                t = t if a == b else t + t
                total = t if total is None else total + t
        return total

    one = jnp.ones((8, 128), F32)
    zero = jnp.zeros((8, 128), F32)
    rho, pi = [one], [one]
    xs = [zero, zero, zero]
    norm = mu[0]
    for n in range(3):
        alpha = norm / quad(pi, stiff)
        for a in range(n + 1):
            xs[a] = xs[a] + alpha * pi[a]
        moved = [(alpha * pi[a] if a <= n else zero) + (alpha * pi[a - 1] if a else zero)
                 for a in range(n + 2)]
        rho = [(rho[a] if a < len(rho) else zero) - moved[a] for a in range(n + 2)]
        if n < 2:
            new = quad(rho, gram)
            beta = new / norm
            pi = [rho[a] + (beta * pi[a] if a < len(pi) else zero) for a in range(n + 2)]
            norm = new

    on_plane = 1.0 - pm
    for k in range(8):
        for j in range(8):
            t = tile(k, j)
            vel[t, :] = (rows(QB, 64 + k * 8 + j) * on_plane + xs[0] * V[0, t, :]
                         + xs[1] * V[1, t, :] + xs[2] * V[2, t, :])
            image = assembled(OUT, 3, k, j) * free(k, j)
            res[t, :] = (rho[0] * SB[0, t, :] + rho[1] * SB[1, t, :]
                         + (rho[2] - rho[3]) * SB[2, t, :] + rho[3] * image)

    for d in range(-2, 3):
        when_there(d, lambda d=d: req_copy(d).wait_send())
    for d in (-1, 1):
        when_there(d, lambda d=d: aux_copy(d).wait_send())
        when_there(d, lambda d=d: halo_copy(FB, 0, d).wait_send())
        when_there(d, lambda d=d: halo_copy(OUT, 3, d).wait_send())
    for f in range(5):
        for s in range(5):
            when_there(2 - s, lambda f=f, s=s: ans_copy(f, s).wait_send())

    for s in range(5):
        for side in range(2):
            @pl.when(tells(s, side))
            def _(s=s, side=side):
                near_copy(s, side).wait_send()

    def left(d, c):
        peer = lax.rem(q + d, NQ)
        pltpu.make_async_remote_copy(
            ar.at[q], ar.at[q], ar_s.at[d], ar_r.at[q],
            device_id=(m, peer), device_id_type=MESH).wait_send()
        return c

    lax.fori_loop(1, NQ, left, 0, unroll=9)


def write_out(vel, res, iv, vel_out, res_out, iv_out, sem):
    copies = [pltpu.make_async_copy(a, b, sem.at[n])
              for n, (a, b) in enumerate(((vel, vel_out), (res, res_out), (iv, iv_out)))]
    for copy in copies:
        copy.start()
    for copy in copies:
        copy.wait()


def body(donor_fields, interp_weights, donor_owner, donor_element, geometry, wall_flag, forcing):
    vm = pl.BlockSpec(memory_space=pltpu.VMEM)
    hbm = pl.BlockSpec(memory_space=pltpu.HBM)
    dma = pltpu.SemaphoreType.DMA
    f32 = lambda *shape: pltpu.VMEM(shape, F32)
    held = pl.pallas_call(
        kernel,
        out_shape=(
            jax.ShapeDtypeStruct((512, 128), F32),
            jax.ShapeDtypeStruct((512, 128), F32),
            jax.ShapeDtypeStruct((5, 2048), F32),
        ),
        in_specs=[hbm] * 8,
        out_specs=(vm, vm, vm),
        scratch_shapes=[
            f32(5, 512, 128), f32(3, 8, 2048), pltpu.VMEM((16, 128), jnp.int32),
            pltpu.VMEM((16, 128), jnp.int32), f32(4, 128), pltpu.VMEM((2, 8), jnp.int32),
            f32(512, 128), f32(96, 128), f32(64, 128), f32(64, 128), f32(5, 64, 128),
            f32(8, 128), f32(2, 8, 128), f32(24 * NB, 128), pltpu.VMEM((NB, 128), jnp.int32),
            pltpu.VMEM((5, 128, 2048), BF16), pltpu.VMEM((5 * HALF, 256), BF16),
            f32(5, NB, 128), f32(5, 5, 16, 128), f32(5, 2, 2, 1, 128), f32(2, 5, 2, 1, 128), f32(16, 128),
            f32(512, 128), f32(512, 128), f32(512, 128),
            f32(3, 512, 128), f32(3, 512, 128), f32(512, 128), f32(128, 128), f32(128, 128),
            f32(4, 2, 64, 128), f32(NQ, 1, 128),
            dma((8,)), dma((5,)), dma((5,)), dma((2,)), dma((2,)), dma((5, 5)), dma((5, 5)),
            dma((5, 2)), dma((2, 5)), dma((4, 2)), dma((4, 2)), dma((NQ,)), dma((NQ,)),
        ],
        compiler_params=pltpu.CompilerParams(
            collective_id=0, has_side_effects=True, vmem_limit_bytes=64500000),
        name="step_window",
    )(
        donor_fields, interp_weights, donor_owner.reshape(16, 128),
        donor_element.reshape(16, 128), geometry, wall_flag, forcing,
        jnp.asarray(const_table()),
    )
    return pl.pallas_call(
        write_out,
        out_shape=tuple(jax.ShapeDtypeStruct(a.shape, F32) for a in held),
        in_specs=[vm] * 3,
        out_specs=(hbm,) * 3,
        scratch_shapes=[dma((3,))],
        name="write_out",
    )(*held)


def solution(mesh):
    both = ("mesh", "dom")
    in_specs = (
        P(None, None, both), P(None, None, both), P(both, None), P(both),
        P(None, both), P(None, both), P(None, both),
    )
    out_specs = (P(None, both), P(None, both), P(None, both))
    return jax.shard_map(body, mesh=mesh, in_specs=in_specs, out_specs=out_specs, check_vma=False)
```

```python
import functools

import jax
import jax.numpy as jnp
import numpy as np
from jax import lax
from jax.experimental import pallas as pl
from jax.experimental.pallas import tpu as pltpu
from jax.sharding import PartitionSpec as P

MESH = pl.DeviceIdType.MESH
F32 = jnp.float32
NQ = 64
NB = 80
KM = 6
HALF = KM * 64
BF16 = jnp.bfloat16


def legendre_pair(values, degree):
    previous = values * 0.0 + 1.0
    current = values * 1.0
    for order in range(2, degree + 1):
        previous, current = (
            current,
            ((2 * order - 1) * values * current - (order - 1) * previous) / order,
        )
    return current, previous


def gll():
    degree, count = 7, 8
    x = np.cos(np.pi * np.arange(count) / degree)
    for _ in range(80):
        top, lower = legendre_pair(x, degree)
        x = x - (x * top - lower) / (count * top)
    x = np.sort(x)
    top, _ = legendre_pair(x, degree)
    w = 2.0 / (degree * count * top * top)
    eye = np.eye(count)
    d = top[:, None] / (top[None, :] * (x[:, None] - x[None, :] + eye)) * (1.0 - eye)
    d[0, 0] = -degree * count / 4.0
    d[7, 7] = degree * count / 4.0
    return x, w, d


X, WQ, D = gll()
KP = (D.T * WQ[None, :]) @ D / WQ[:, None]
KP = 0.5 * (KP + KP[::-1, ::-1])
KE = 0.5 * (KP[:4, :4] + KP[:4, 7:3:-1])
KO = 0.5 * (KP[:4, :4] - KP[:4, 7:3:-1])
LC = np.array([1.0 / np.prod([X[n] - X[m] for m in range(8) if m != n]) for n in range(8)])


def const_table():
    lane = np.arange(128)
    xl = lane % 8
    rows = []
    rows.append(np.repeat(X[:, None], 128, 1))
    rows.append(np.repeat(WQ[:, None], 128, 1))
    for s in range(8):
        rows.append(np.repeat(np.array([KP[i, (i + s) % 8] for i in range(8)])[:, None], 128, 1))
    kx = np.zeros((8, 128))
    for i in range(8):
        kx[i] = np.where(xl == 0, KP[i, 0], np.where(xl == 7, KP[i, 7], 0.0))
    kx[0] = np.where(xl == 1, KP[7, 0], kx[0])
    kx[7] = np.where(xl == 6, KP[0, 7], kx[7])
    rows.append(kx)
    rows.append((np.arange(8)[:, None] == xl[None, :]).astype(float))
    return np.concatenate(rows, 0).astype(np.float32)


def kernel(
    donor_hbm, wts_hbm, owner_hbm, elem_hbm, geo_hbm, wall_hbm, forc_hbm, ct_hbm,
    vel_hbm, res_hbm, iv_hbm,
    donor, wts, owner, elem, geo, wall, forc, ct, nat, req_src, req, aux_src, aux, W, IDX, OH, DB,
    ans_src, ans, fbuf, nbf, got,
    FB, OUT, INV, V, SB, DG, ND, QB, halo, ar, vel, res, iv, out_sem,
    in_sem, req_s, req_r, aux_s, aux_r, ans_s, ans_r, nb_s, nb_r, halo_s, halo_r, ar_s, ar_r,
):
    m = lax.axis_index("mesh")
    q = lax.axis_index("dom")
    om = 1 - m
    barrier = pltpu.get_barrier_semaphore()

    def there(d):
        return jnp.logical_and(q + d >= 0, q + d < NQ)

    pairs = ((wts_hbm, wts), (ct_hbm, ct), (owner_hbm, owner), (elem_hbm, elem), (geo_hbm, geo),
             (wall_hbm, wall), (forc_hbm, forc), (donor_hbm, donor))
    loads = [pltpu.make_async_copy(a, b, in_sem.at[n]) for n, (a, b) in enumerate(pairs)]
    for load in loads:
        load.start()

    for d, s in ((-1, 0), (1, 1)):
        @pl.when(jnp.logical_not(there(d)))
        def _(s=s):
            aux[s] = jnp.zeros((8, 128), F32)
            for r in range(4):
                halo[r, s] = jnp.zeros((64, 128), F32)
    for d in (-2, -1, 1, 2):
        @pl.when(jnp.logical_not(there(d)))
        def _(d=d):
            req[2 - d] = jnp.zeros((64, 128), F32)
            ans[2 + d] = jnp.zeros((5, 16, 128), F32)

    def hears(side, s):
        r = 2 * side - 1
        return jnp.logical_and(there(r), there(r + s - 2))

    for side in range(2):
        for s in range(5):
            @pl.when(jnp.logical_not(hears(side, s)))
            def _(side=side, s=s):
                nbf[side, s] = jnp.zeros((2, 1, 128), F32)

    def greet(d, c):
        peer = lax.rem(q + d, NQ)
        pl.semaphore_signal(barrier, inc=1, device_id=(m, peer), device_id_type=MESH)
        return c

    lax.fori_loop(1, NQ, greet, 0, unroll=9)
    for d in range(-3, 4):
        @pl.when(there(d))
        def _(d=d):
            pl.semaphore_signal(barrier, inc=1, device_id=(om, q + d), device_id_type=MESH)

    i0 = lax.broadcasted_iota(jnp.int32, (8, 128), 0)
    lane = lax.broadcasted_iota(jnp.int32, (8, 128), 1)
    xl = lane & 7
    yl = lane >> 3
    for load in loads[:6]:
        load.wait()
    xcol = ct[0:8, :]
    wcol = ct[8:16, :]

    for d in range(3):
        for b in range(16):
            t = wts[d, :, b * 128 : (b + 1) * 128] * xcol
            nat[d * 16 + b : d * 16 + b + 1, :] = jnp.sum(t, axis=0, keepdims=True)
    nat[48:64, :] = (owner[...] * 128 + elem[...]).astype(F32)

    def lanes(value, at):
        return jnp.take_along_axis(value, at, axis=1, mode="promise_in_bounds")

    from_y = lane >> 4 == i0
    for d in range(4):
        for s in range(2):
            a = nat[d * 16 + s * 8 : d * 16 + s * 8 + 8, :]
            for k in range(8):
                t = lanes(a, ((lane >> 3) & 1) * 64 + k * 8 + (lane & 7))
                at = d * 16 + k * 2 + s
                req_src[at : at + 1, :] = jnp.sum(
                    jnp.where(from_y, t, 0.0), axis=0, keepdims=True)
    aux_src[0:4, :] = geo[...]
    aux_src[4:6, :] = jnp.dot(
        wall[...].astype(F32), ct[88:96, :], preferred_element_type=F32
    )
    aux_src[6:8, :] = jnp.zeros((2, 128), F32)

    def req_copy(d):
        return pltpu.make_async_remote_copy(
            req_src, req.at[d + 2], req_s.at[d + 2], req_r.at[d + 2],
            device_id=(om, q + d), device_id_type=MESH)

    def aux_copy(d):
        s = (d + 1) // 2
        return pltpu.make_async_remote_copy(
            aux_src, aux.at[1 - s], aux_s.at[s], aux_r.at[1 - s],
            device_id=(m, q + d), device_id_type=MESH)

    def halo_copy(src, r, d):
        s = (d + 1) // 2
        return pltpu.make_async_remote_copy(
            src.at[pl.ds(s * 448, 64)], halo.at[r, 1 - s], halo_s.at[r, s], halo_r.at[r, 1 - s],
            device_id=(m, q + d), device_id_type=MESH)

    def near_copy(s, side):
        return pltpu.make_async_remote_copy(
            fbuf.at[s, side], nbf.at[1 - side, s], nb_s.at[s, side], nb_r.at[1 - side, s],
            device_id=(om, q + 1 - s + 2 * side), device_id_type=MESH)

    def tells(s, side):
        return jnp.logical_and(there(2 - s), there(1 - s + 2 * side))

    def ans_copy(f, s):
        d = 2 - s
        at = s * 16 if isinstance(s, int) else pl.multiple_of(s * 16, 16)
        return pltpu.make_async_remote_copy(
            ans_src.at[f, pl.ds(at, 16)], ans.at[s, f], ans_s.at[f, s], ans_r.at[f, s],
            device_id=(om, q + d), device_id_type=MESH)

    def when_there(d, act):
        @pl.when(there(d))
        def _():
            act()

    m7x = jnp.logical_and(i0 == 7, xl < 7)
    m0x = jnp.logical_and(i0 == 0, xl > 0)
    m7y = jnp.logical_and(i0 == 7, yl < 15)
    m0y = jnp.logical_and(i0 == 0, yl > 0)
    xhi, xlo = xl < 7, xl > 0
    yhi, ylo = yl < 15, yl > 0

    def sum_xy(ref, base, planes):
        for k in range(planes):
            lo = ref[pl.ds(base + k * 64, 8, stride=8), :]
            hi = ref[pl.ds(base + k * 64 + 7, 8, stride=8), :]
            ref[pl.ds(base + k * 64, 8, stride=8), :] = lo + jnp.where(
                xlo, pltpu.roll(hi, 1, axis=1), 0.0)
            ref[pl.ds(base + k * 64 + 7, 8, stride=8), :] = hi + jnp.where(
                xhi, pltpu.roll(lo, 127, axis=1), 0.0)
        for k in range(planes):
            at = base + k * 64
            lo = ref[at : at + 8, :]
            hi = ref[at + 56 : at + 64, :]
            ref[at : at + 8, :] = lo + jnp.where(ylo, pltpu.roll(hi, 8, axis=1), 0.0)
            ref[at + 56 : at + 64, :] = hi + jnp.where(yhi, pltpu.roll(lo, 120, axis=1), 0.0)

    def rows(ref, n):
        return jnp.broadcast_to(ref[n : n + 1, :], (8, 128))

    g0, g1, g2, g3 = (rows(geo, n) for n in range(4))

    def tile(k, j):
        at = (k * 8 + j) * 8
        return slice(at, at + 8)

    def wkj(k, j):
        return float(WQ[k] * WQ[j])

    loads[7].wait()
    for f in range(1):
        for at in range(0, HALF, 64):
            value = donor[f, at : at + 64, :]
            high = value.astype(BF16)
            DB[f * HALF + at : f * HALF + at + 64, 0:128] = high
            DB[f * HALF + at : f * HALF + at + 64, 128:256] = (
                value - high.astype(F32)).astype(BF16)

    loads[6].wait()
    g3w = g3 * wcol
    for k in range(8):
        for j in range(8):
            FB[tile(k, j), :] = forc[tile(k, j), :] * (g3w * wkj(k, j))
    sum_xy(FB, 0, 8)

    width = sum(there(d).astype(jnp.int32) for d in range(-3, 4))
    pl.semaphore_wait(barrier, NQ - 1 + width)
    for d in (0, 1, -1, 2, -2):
        when_there(d, lambda d=d: req_copy(d).start())
    for d in (-1, 1):
        when_there(d, lambda d=d: aux_copy(d).start())
    kdiag = ct[16:24, :]

    def diag_tile(h0, h1, h2, h3, k, j):
        return (h0 * kdiag + h1 * float(KP[j, j]) + h2 * float(KP[k, k]) + h3) * (
            wcol * wkj(k, j))

    for k in range(8):
        for j in range(8):
            DG[tile(k, j), :] = diag_tile(g0, g1, g2, g3, k, j)
    sum_xy(DG, 0, 8)

    for f in range(1, 5):
        for at in range(0, HALF, 64):
            value = donor[f, at : at + 64, :]
            high = value.astype(BF16)
            DB[f * HALF + at : f * HALF + at + 64, 0:128] = high
            DB[f * HALF + at : f * HALF + at + 64, 128:256] = (
                value - high.astype(F32)).astype(BF16)

    plane = jnp.logical_or(
        jnp.logical_and(i0 == 0, xl == 0), jnp.logical_and(i0 == 7, xl == 7))
    pm = jnp.where(plane, 0.0, 1.0)

    def wall_count(row):
        return (row + jnp.where(m7x, pltpu.roll(row, 127, axis=1), 0.0)
                + jnp.where(m0x, pltpu.roll(row, 1, axis=1), 0.0))

    masks = {}
    edges = ((0, yl == 0), (7, yl == 15))

    def wall_mask(j, name, count):
        edge = edges[j // 7][1]
        masks[j, name] = pm * (1.0 - jnp.where(edge, jnp.minimum(count, 1.0), 0.0))

    own = [wall_count(rows(aux_src, 4 + n)) for n in range(2)]
    for n in range(2):
        wall_mask(7 * n, "in", own[n])

    def free(k, j):
        if j not in (0, 7):
            return pm
        return masks[j, "lo" if k == 0 else "hi" if k == 7 else "in"]

    for k in range(1, 7):
        for j in range(8):
            INV[tile(k, j), :] = free(k, j) / DG[tile(k, j), :]

    row_of = lax.broadcasted_iota(jnp.int32, (128, 128), 0)

    def weights(s):
        for h in range(2):
            at = s * 16 + 8 * h
            code = req[s, 48 + 8 * h : 56 + 8 * h, :] - (q * 128).astype(F32)
            mine = jnp.logical_and(code >= 0.0, code < 128.0)
            IDX[pl.ds(pl.multiple_of(at, 8), 8), :] = jnp.where(mine, code, 0.0).astype(jnp.int32)
            keep = jnp.where(mine, 1.0, 0.0)
            for d in range(3):
                xi = req[s, d * 16 + 8 * h : d * 16 + 8 * h + 8, :]
                t = [xi - float(X[n]) for n in range(8)]
                pre, suf = [None], [None] * 8
                for n in range(1, 8):
                    pre.append(t[n - 1] if n == 1 else pre[-1] * t[n - 1])
                for n in range(6, -1, -1):
                    suf[n] = t[7] if n == 6 else suf[n + 1] * t[n + 1]
                for n in range(8):
                    a = suf[0] if n == 0 else pre[7] if n == 7 else pre[n] * suf[n]
                    a = a * float(LC[n])
                    if d == 0:
                        a = a * keep
                    W[pl.ds(pl.multiple_of((s * 24 + d * 8 + n) * 16 + 8 * h, 8), 8), :] = a
        for u in range(16):
            column = jnp.broadcast_to(IDX[pl.ds(s * 16 + u, 1), :], (128, 128))
            OH[s, :, u * 128 : (u + 1) * 128] = jnp.where(
                row_of == column, 1.0, 0.0).astype(BF16)

    def evaluate(fields, s):
        hot = OH[s]
        hot = jnp.concatenate([hot, hot], axis=0)
        picked = {}
        for f in fields:
            picked[f] = jnp.dot(DB[f * HALF : (f + 1) * HALF, :], hot, preferred_element_type=F32)
        base = s * 384
        for f in fields:
            for u in range(16):
                idx = jnp.broadcast_to(IDX[pl.ds(s * 16 + u, 1), :], (8, 128))
                wi = W[pl.ds(base + u, 8, stride=16), :]
                wj = [jnp.broadcast_to(W[pl.ds(base + (8 + j) * 16 + u, 1), :], (8, 128))
                      for j in range(8)]
                total = None
                for k in range(8):
                    wk = jnp.broadcast_to(W[pl.ds(base + (16 + k) * 16 + u, 1), :], (8, 128))
                    part = None
                    for j in range(8):
                        t = tile(k, j)
                        if k < KM:
                            g = picked[f][t, u * 128 : (u + 1) * 128]
                        else:
                            g = lanes(donor[f, t, :], idx)
                        part = g * wj[j] if part is None else part + g * wj[j]
                    total = part * wk if total is None else total + part * wk
                line = jnp.sum(total * wi, axis=0, keepdims=True)
                ans_src[f, pl.ds(s * 16 + u, 1), :] = line
                if f == 0 and u in (0, 1, 14, 15):
                    fbuf[s, u // 14, u % 2] = line

    def all_slots(fields):
        def step(s, c):
            evaluate(fields, s)
            return c

        lax.fori_loop(0, 5, step, 0, unroll=5)
        for f in fields:
            for s in (0, 4, 1, 3, 2):
                when_there(2 - s, lambda f=f, s=s: ans_copy(f, s).start())

    def serve(n, c):
        s = 2 + ((n + 1) // 2) * (1 - 2 * (n % 2))
        when_there(2 - s, lambda: req_copy(s - 2).wait_recv())
        weights(s)
        evaluate((0,), s)
        when_there(2 - s, lambda: ans_copy(0, s).start())
        for side in range(2):
            @pl.when(tells(s, side))
            def _(side=side):
                near_copy(s, side).start()
        return c

    lax.fori_loop(0, 5, serve, 0)
    for d in (-1, 1):
        when_there(d, lambda d=d: halo_copy(FB, 0, d).start())
    for d, s in ((-1, 0), (1, 1)):
        when_there(d, lambda d=d, s=s: aux_copy(-d).wait_recv())

    for n in range(2):
        for s, name in ((0, "lo"), (1, "hi")):
            other = wall_count(jnp.broadcast_to(aux[s, 4 + n : 5 + n, :], (8, 128)))
            wall_mask(7 * n, name, own[n] + other)

    for s in range(2):
        h = [jnp.broadcast_to(aux[s, n : n + 1, :], (8, 128)) for n in range(4)]
        for j in range(8):
            ND[s * 64 + j * 8 : s * 64 + j * 8 + 8, :] = diag_tile(*h, 0, j)
    sum_xy(ND, 0, 2)
    for k in (0, 7):
        for j in range(8):
            value = DG[tile(k, j), :] + ND[tile(k // 7, j), :]
            INV[tile(k, j), :] = free(k, j) / value

    all_slots((1, 2))

    for s in range(5):
        when_there(s - 2, lambda s=s: ans_copy(0, s).wait_recv())
    for side in range(2):
        for s in range(5):
            @pl.when(hears(side, s))
            def _(side=side, s=s):
                near_copy(s, 1 - side).wait_recv()
    got[...] = ans[0, 0] + ans[1, 0] + ans[2, 0] + ans[3, 0] + ans[4, 0]

    def on_planes(low, high):
        at = yl * 8 + i0
        t = jnp.where(xl == 0, lanes(jnp.broadcast_to(low, (8, 128)), at),
                      jnp.where(xl == 7, lanes(jnp.broadcast_to(high, (8, 128)), at), 0.0))
        return (t + jnp.where(m7y, pltpu.roll(pltpu.roll(t, 120, axis=1), 7, axis=0), 0.0)
                + jnp.where(m0y, pltpu.roll(pltpu.roll(t, 8, axis=1), 1, axis=0), 0.0))

    T = [on_planes(got[2 * k : 2 * k + 1, :], got[2 * k + 1 : 2 * k + 2, :]) for k in range(8)]
    for side, k in ((0, 0), (1, 7)):
        low, high = (sum(nbf[side, s, n] for s in range(1, 5)) + nbf[side, 0, n]
                     for n in range(2))
        T[k] = T[k] + on_planes(low, high)
    czd = jnp.where(q > 0, 0.5, 1.0).astype(F32)
    czu = jnp.where(q < NQ - 1, 0.5, 1.0).astype(F32)
    cyv = jnp.where(jnp.logical_or(m7y, m0y), 0.5, 1.0)

    def spread_y(row):
        return (row + jnp.where(m7y, pltpu.roll(row, 120, axis=1), 0.0)
                + jnp.where(m0y, pltpu.roll(row, 8, axis=1), 0.0))

    gy = spread_y(g0)
    gy_below = spread_y(jnp.broadcast_to(aux[0, 0:1, :], (8, 128)))
    gy_above = spread_y(jnp.broadcast_to(aux[1, 0:1, :], (8, 128)))
    for k in range(8):
        b = T[k] * cyv
        gs = gy
        if k == 0:
            b, gs = b * czd, gs + gy_below
        if k == 7:
            b, gs = b * czu, gs + gy_above
        QB[64 + k * 8 : 72 + k * 8, :] = b
        t = b * gs
        t = jnp.where(xl == 1, pltpu.roll(t, 1, axis=1),
                      jnp.where(xl == 6, pltpu.roll(t, 127, axis=1), t))
        QB[k * 8 : k * 8 + 8, :] = t

    cx = jnp.where(jnp.logical_or(m7x, m0x), 0.5, 1.0)
    cxy = {0: cx * jnp.where(ylo, 0.5, 1.0), 7: cx * jnp.where(yhi, 0.5, 1.0)}

    def assembled(src, r, k, j):
        value = src[tile(k, j), :]
        if k == 0:
            value = value + halo[r, 0, j * 8 : j * 8 + 8, :]
        if k == 7:
            value = value + halo[r, 1, j * 8 : j * 8 + 8, :]
        return value

    def wait_halo(src, r):
        for d in (-1, 1):
            when_there(d, lambda d=d: halo_copy(src, r, -d).wait_recv())

    def inner_sums(make, count, planes=range(8)):
        totals = [None] * count
        for k in planes:
            parts = [None] * count
            for j in range(8):
                one, others = make(k, j)
                one = one * cxy.get(j, cx)
                for n, other in enumerate(others):
                    t = one * other
                    parts[n] = t if parts[n] is None else parts[n] + t
            for n in range(count):
                t = parts[n]
                if k == 0:
                    t = t * czd
                if k == 7:
                    t = t * czu
                totals[n] = t if totals[n] is None else totals[n] + t
        return totals

    kxw = ct[80:88, :] * wcol
    wait_halo(FB, 0)

    def first(k, j):
        value = assembled(FB, 0, k, j) - rows(QB, k * 8 + j) * (kxw * wkj(k, j))
        value = value * free(k, j)
        SB[0, tile(k, j), :] = value
        pre = value * INV[tile(k, j), :]
        V[0, tile(k, j), :] = pre
        return pre, (value,)

    moments = inner_sums(first, 1)

    kroll = [ct[16 + 8 * s : 24 + 8 * s, :] for s in range(8)]

    def eight(v):
        e = [v[n] + v[7 - n] for n in range(4)]
        o = [v[n] - v[7 - n] for n in range(4)]
        out = [None] * 8
        for n in range(4):
            a, b = None, None
            for c in range(4):
                ta, tb = e[c] * float(KE[n, c]), o[c] * float(KO[n, c])
                a = ta if a is None else a + ta
                b = tb if b is None else b + tb
            out[n], out[7 - n] = a + b, a - b
        return out

    def ends_of_eight(v):
        a, b = None, None
        for c in range(4):
            ta, tb = (v[c] + v[7 - c]) * float(KE[0, c]), (v[c] - v[7 - c]) * float(KO[0, c])
            a = ta if a is None else a + ta
            b = tb if b is None else b + tb
        return {0: a + b, 7: a - b}

    def local_operator(src, dst, planes, wanted):
        faces = len(planes) == 2
        for j in range(8):
            v = [src[tile(k, j), :] for k in range(8)]
            z = ends_of_eight(v) if faces else eight(v)
            for k in planes:
                dst[tile(k, j), :] = z[k] * g2 + v[k] * g3
        energy = None
        for k in planes:
            v = [src[tile(k, j), :] for j in range(8)]
            y = eight(v)
            for j in range(8):
                x = v[j] * kroll[0]
                for s in range(1, 8):
                    x = x + pltpu.roll(v[j], 8 - s, axis=0) * kroll[s]
                value = (dst[tile(k, j), :] + y[j] * g1 + x * g0) * (wcol * wkj(k, j))
                dst[tile(k, j), :] = value
                if wanted:
                    t = v[j] * value
                    energy = t if energy is None else energy + t
        return energy

    def fold(n, planes):
        def make(k, j):
            t = tile(k, j)
            value = assembled(OUT, n + 1, k, j) * free(k, j) - SB[n, t, :]
            SB[n + 1, t, :] = value
            pre = value * INV[t, :]
            V[n + 1, t, :] = pre
            return pre, tuple(SB[a, t, :] for a in range(n + 1)) + (value,)

        return inner_sums(make, n + 2, planes)

    row = [jnp.zeros((1, 128), F32), 0]
    lane_of = lax.broadcasted_iota(jnp.int32, (1, 128), 1)

    def collect():
        while row[1] < len(moments):
            t = jnp.sum(jnp.sum(moments[row[1]], axis=0, keepdims=True), axis=1, keepdims=True)
            row[0] = jnp.where(lane_of == row[1], t, row[0])
            row[1] += 1
        return row[0]

    for n in range(2):
        local_operator(V.at[n], OUT, (0, 7), False)
        sum_xy(OUT, 0, 1)
        sum_xy(OUT, 448, 1)
        for d in (-1, 1):
            when_there(d, lambda d=d: halo_copy(OUT, n + 1, d).start())
        local_operator(V.at[n], OUT, range(1, 7), False)
        sum_xy(OUT, 64, 6)
        inside = fold(n, range(1, 7))
        collect()
        all_slots((3 + n,))
        wait_halo(OUT, n + 1)
        for d in (-1, 1):
            when_there(d, lambda d=d: halo_copy(OUT, n + 1, d).wait_send())
        moments.extend(a + b for a, b in zip(inside, fold(n, (0, 7))))

    moments.append(local_operator(V.at[2], OUT, range(8), True))
    ar[q] = collect()

    def tell(d, c):
        peer = lax.rem(q + d, NQ)
        pltpu.make_async_remote_copy(
            ar.at[q], ar.at[q], ar_s.at[d], ar_r.at[q],
            device_id=(m, peer), device_id_type=MESH).start()
        return c

    lax.fori_loop(1, NQ, tell, 0, unroll=9)
    sum_xy(OUT, 0, 8)
    for d in (-1, 1):
        when_there(d, lambda d=d: halo_copy(OUT, 3, d).start())

    for f in range(1, 5):
        for s in range(5):
            when_there(s - 2, lambda f=f, s=s: ans_copy(f, s).wait_recv())
    from_k = (lane >> 3) & 7 == i0
    for f in range(5):
        for s in range(2):
            a = (ans[0, f, pl.ds(s, 8, stride=2), :] + ans[1, f, pl.ds(s, 8, stride=2), :]
                 + ans[2, f, pl.ds(s, 8, stride=2), :] + ans[3, f, pl.ds(s, 8, stride=2), :]
                 + ans[4, f, pl.ds(s, 8, stride=2), :])
            for y in range(8):
                t = lanes(a, y * 16 + (lane >> 6) * 8 + (lane & 7))
                at = (s * 8 + y) * 128
                iv[f : f + 1, at : at + 128] = jnp.sum(
                    jnp.where(from_k, t, 0.0), axis=0, keepdims=True)

    outs = [pltpu.make_async_copy(iv, iv_hbm, out_sem.at[4])]
    outs[0].start()

    for d in range(-2, 3):
        when_there(d, lambda d=d: req_copy(d).wait_send())
    for d in (-1, 1):
        when_there(d, lambda d=d: aux_copy(d).wait_send())
        when_there(d, lambda d=d: halo_copy(FB, 0, d).wait_send())
        when_there(d, lambda d=d: halo_copy(OUT, 3, d).wait_send())
    for f in range(5):
        for s in range(5):
            when_there(2 - s, lambda f=f, s=s: ans_copy(f, s).wait_send())

    for s in range(5):
        for side in range(2):
            @pl.when(tells(s, side))
            def _(s=s, side=side):
                near_copy(s, side).wait_send()

    def left(d, c):
        peer = lax.rem(q + d, NQ)
        pltpu.make_async_remote_copy(
            ar.at[q], ar.at[q], ar_s.at[d], ar_r.at[q],
            device_id=(m, peer), device_id_type=MESH).wait_send()
        return c

    lax.fori_loop(1, NQ, left, 0, unroll=9)

    wait_halo(OUT, 3)

    def hear(d, c):
        peer = lax.rem(q + d, NQ)
        pltpu.make_async_remote_copy(
            ar.at[peer], ar.at[peer], ar_s.at[d], ar_r.at[peer],
            device_id=(m, peer), device_id_type=MESH).wait_recv()
        return c

    lax.fori_loop(1, NQ, hear, 0, unroll=9)
    parts = [ar[n] for n in range(NQ)]
    while len(parts) > 1:
        parts = [parts[n] + parts[n + 1] for n in range(0, len(parts), 2)]
    sums = jnp.broadcast_to(parts[0], (8, 128))
    mu = [
        jnp.take_along_axis(sums, jnp.full((8, 128), n, jnp.int32), axis=1,
                            mode="promise_in_bounds")
        for n in range(7)
    ]

    gram = {(0, 0): mu[0], (0, 1): mu[1], (1, 1): mu[2], (0, 2): mu[3], (1, 2): mu[4],
            (2, 2): mu[5]}
    stiff = {(0, 0): mu[1] + mu[0], (0, 1): mu[2] + mu[1], (1, 1): mu[4] + mu[2],
             (0, 2): mu[4] + mu[3], (1, 2): mu[5] + mu[4], (2, 2): mu[6]}

    def quad(c, form):
        total = None
        for a in range(len(c)):
            for b in range(a, len(c)):
                t = c[a] * c[b] * form[a, b]
                t = t if a == b else t + t
                total = t if total is None else total + t
        return total

    one = jnp.ones((8, 128), F32)
    zero = jnp.zeros((8, 128), F32)
    rho, pi = [one], [one]
    xs = [zero, zero, zero]
    norm = mu[0]
    for n in range(3):
        alpha = norm / quad(pi, stiff)
        for a in range(n + 1):
            xs[a] = xs[a] + alpha * pi[a]
        moved = [(alpha * pi[a] if a <= n else zero) + (alpha * pi[a - 1] if a else zero)
                 for a in range(n + 2)]
        rho = [(rho[a] if a < len(rho) else zero) - moved[a] for a in range(n + 2)]
        if n < 2:
            new = quad(rho, gram)
            beta = new / norm
            pi = [rho[a] + (beta * pi[a] if a < len(pi) else zero) for a in range(n + 2)]
            norm = new

    on_plane = 1.0 - pm
    for k in range(8):
        for j in range(8):
            t = tile(k, j)
            vel[t, :] = (rows(QB, 64 + k * 8 + j) * on_plane + xs[0] * V[0, t, :]
                         + xs[1] * V[1, t, :] + xs[2] * V[2, t, :])
            image = assembled(OUT, 3, k, j) * free(k, j)
            res[t, :] = (rho[0] * SB[0, t, :] + rho[1] * SB[1, t, :]
                         + (rho[2] - rho[3]) * SB[2, t, :] + rho[3] * image)
        if k % 4 == 3:
            at = pl.ds(k // 4 * 256, 256)
            for n, (a, b) in enumerate(((vel, vel_hbm), (res, res_hbm))):
                outs.append(pltpu.make_async_copy(a.at[at], b.at[at], out_sem.at[k // 4 * 2 + n]))
                outs[-1].start()
    for copy in outs:
        copy.wait()


def write_out(vel, res, iv, vel_out, res_out, iv_out, sem):
    copies = [pltpu.make_async_copy(a, b, sem.at[n])
              for n, (a, b) in enumerate(((vel, vel_out), (res, res_out), (iv, iv_out)))]
    for copy in copies:
        copy.start()
    for copy in copies:
        copy.wait()


def body(donor_fields, interp_weights, donor_owner, donor_element, geometry, wall_flag, forcing):
    vm = pl.BlockSpec(memory_space=pltpu.VMEM)
    hbm = pl.BlockSpec(memory_space=pltpu.HBM)
    dma = pltpu.SemaphoreType.DMA
    f32 = lambda *shape: pltpu.VMEM(shape, F32)
    held = pl.pallas_call(
        kernel,
        out_shape=(
            jax.ShapeDtypeStruct((512, 128), F32),
            jax.ShapeDtypeStruct((512, 128), F32),
            jax.ShapeDtypeStruct((5, 2048), F32),
        ),
        in_specs=[hbm] * 8,
        out_specs=(hbm, hbm, hbm),
        scratch_shapes=[
            f32(5, 512, 128), f32(3, 8, 2048), pltpu.VMEM((16, 128), jnp.int32),
            pltpu.VMEM((16, 128), jnp.int32), f32(4, 128), pltpu.VMEM((2, 8), jnp.int32),
            f32(512, 128), f32(96, 128), f32(64, 128), f32(64, 128), f32(5, 64, 128),
            f32(8, 128), f32(2, 8, 128), f32(24 * NB, 128), pltpu.VMEM((NB, 128), jnp.int32),
            pltpu.VMEM((5, 128, 2048), BF16), pltpu.VMEM((5 * HALF, 256), BF16),
            f32(5, NB, 128), f32(5, 5, 16, 128), f32(5, 2, 2, 1, 128), f32(2, 5, 2, 1, 128), f32(16, 128),
            f32(512, 128), f32(512, 128), f32(512, 128),
            f32(3, 512, 128), f32(3, 512, 128), f32(512, 128), f32(128, 128), f32(128, 128),
            f32(4, 2, 64, 128), f32(NQ, 1, 128), f32(512, 128), f32(512, 128), f32(5, 2048), dma((5,)),
            dma((8,)), dma((5,)), dma((5,)), dma((2,)), dma((2,)), dma((5, 5)), dma((5, 5)),
            dma((5, 2)), dma((2, 5)), dma((4, 2)), dma((4, 2)), dma((NQ,)), dma((NQ,)),
        ],
        compiler_params=pltpu.CompilerParams(
            collective_id=0, has_side_effects=True, vmem_limit_bytes=64500000),
        name="step_window",
    )(
        donor_fields, interp_weights, donor_owner.reshape(16, 128),
        donor_element.reshape(16, 128), geometry, wall_flag, forcing,
        jnp.asarray(const_table()),
    )
    return pl.pallas_call(
        write_out,
        out_shape=tuple(jax.ShapeDtypeStruct(a.shape, F32) for a in held),
        in_specs=[vm] * 3,
        out_specs=(hbm,) * 3,
        scratch_shapes=[dma((3,))],
        name="write_out",
    )(*held)


def solution(mesh):
    both = ("mesh", "dom")
    in_specs = (
        P(None, None, both), P(None, None, both), P(both, None), P(both),
        P(None, both), P(None, both), P(None, both),
    )
    out_specs = (P(None, both), P(None, both), P(None, both))
    return jax.shard_map(body, mesh=mesh, in_specs=in_specs, out_specs=out_specs, check_vma=False)
```
